32 devices in a mesh: dp: 4 (over z), seq: 8 (over y, x, core).
Axes of the slice: x: 2, y: 2, z: 4, core: 2. Of those that a mesh axis runs over, the one named last changes fastest.
Arguments:
- projections: bfloat16 [1, 4, 1024, 4096], P(None, 'dp', 'seq'), may hold values from -6 to 6
- rotated_query_gradient: bfloat16 [1, 4, 1024, 4096], P(None, 'dp', None, 'seq'), may hold values from -6 to 6
- gains: float32 [1, 4096], replicated, may hold values from 0.25 to 1.75
- adapter_lowering: bfloat16 [1, 48, 5120], P(None, 'dp'), may hold values from -0.078125 to 0.078125
- adapter_raising: bfloat16 [1, 48, 4096], P(None, 'dp'), may hold values from -0.875 to 0.875
- activations: bfloat16 [4, 1024, 5120], P('dp', 'seq'), may hold values from -6 to 6
- positions: int32 [3, 4, 1024], P(None, 'dp', 'seq'), may hold values from 0 to 22, as said below
- valid: int32 [4, 1024], P('dp', 'seq'), may hold values from 0 to 1, as said below
Outputs:
- grad_down: float32 [1, 48, 5120], P(None, 'dp')
- grad_up: float32 [1, 48, 4096], P(None, 'dp')
- grad_gain: float32 [1, 4096], replicated
The draws below stay inside these ranges and needn't reach their ends.
Inputs may be any that keep to these rules, and one draw needn't show every extreme that they name: `positions`: within a video the frame index never falls; one frame holds 128 tokens. Every eighth token of a video is valid.
All inputs are finite; a program needn't handle non-finite values.
Results may differ from the reference program's by a relative error of at most 0.0041.
Values may be sent and summed in bfloat16 or wider, within the bound.
A program may use at most 64 MiB of HBM per device.

```python
import jax
import jax.numpy as jnp
from jax import lax

MODEL_WIDTH = 5120
HD = 128
ADAPTER_RANK = 48
QUERY_FEATURES = 4096
LEN = 1024
SAMPLES = 4


def draw_positions(key, part):
    token_index = jnp.arange(LEN, dtype=jnp.int32)
    offsets = jax.random.randint(key, (3, SAMPLES, 1), 0, 8)
    sample_index = jnp.arange(SAMPLES, dtype=jnp.int32)[None, :, None]
    offsets = jnp.where(sample_index == 0, 0, offsets)
    offsets = jnp.where(sample_index == SAMPLES - 1, 7, offsets)
    grid_base = jnp.stack([token_index // 128, token_index // 16 % 8, token_index % 16])[:, None, :]
    return (grid_base + offsets).astype(jnp.int32)


def draw_valid(key, part):
    token_index = jnp.arange(LEN, dtype=jnp.int32)
    draw_level = jax.random.randint(key, (SAMPLES, LEN), 0, 1000)
    kept_rows = draw_level < 300 + 600 * token_index // LEN
    return jnp.where((token_index % 8 == 0) | kept_rows, 1, 0).astype(jnp.int32)


def levels(rng, extent, shards, least, largest):
    gain = 1.0
    for dim, blocks in shards:
        heights = jax.random.uniform(jax.random.fold_in(jax.random.fold_in(rng, 6), dim), (blocks,), jnp.float32, least / len(shards), largest / len(shards))
        gain = gain * jnp.repeat(jnp.exp(heights), extent[dim] // blocks).reshape((-1,) + (1,) * (len(extent) - 1 - dim))
    return gain


def noise(key, dims, spread, bound, cuts=(), held_as=jnp.bfloat16):
    values = jax.random.normal(key, dims, jnp.float32) * spread
    if len(cuts) > 0:
        values = levels(key, dims, cuts, -0.22, 0.18) * values
    return jnp.clip(values, min=-bound, max=bound).astype(held_as)


def setup_inputs(seed: int = 0) -> dict:
    seeds = jax.random.split(jax.random.key(seed), 9)
    projections = noise(seeds[0], (1, SAMPLES, LEN, QUERY_FEATURES), 1.0, 6.0, ((1, 4), (2, 8)))
    rotated_query_gradient = noise(seeds[1], (1, SAMPLES, LEN, QUERY_FEATURES), 1.0, 6.0, ((1, 4), (3, 8)))
    gains = jnp.clip(1.0 + 0.15 * jax.random.normal(seeds[2], (1, QUERY_FEATURES), jnp.float32), 0.25, 1.75)
    adapter_lowering = noise(seeds[3], (1, ADAPTER_RANK, MODEL_WIDTH), MODEL_WIDTH ** -0.5, 0.078125, ((1, 4),))
    adapter_raising = noise(seeds[4], (1, ADAPTER_RANK, QUERY_FEATURES), ADAPTER_RANK ** -0.5, 0.875, ((1, 4),))
    activations = noise(seeds[5], (SAMPLES, LEN, MODEL_WIDTH), 1.0, 6.0, ((0, 4), (1, 8)))
    positions = draw_positions(jax.random.fold_in(seeds[8], 71), 0)
    valid = draw_valid(jax.random.fold_in(seeds[8], 71), 0)
    return {"projections": projections, "rotated_query_gradient": rotated_query_gradient, "gains": gains, "adapter_lowering": adapter_lowering, "adapter_raising": adapter_raising, "activations": activations, "positions": positions, "valid": valid}


EPSILON = 1e-06

def rope_tables(positions, head_size):
    one_sixth = head_size // 6
    counts = (head_size // 2 - 2 * one_sixth, one_sixth, one_sixth)
    pieces = []
    for component in range(3):
        frequency = 10000.0 ** (-jnp.arange(counts[component], dtype=jnp.float32) / counts[component])
        pieces.append(positions[component].astype(jnp.float32)[..., None] * frequency)
    angles = jnp.concatenate(pieces, -1)
    return (jnp.cos(angles), jnp.sin(angles))

def norm_backward(projections, rotated_query_gradient, gains, positions, valid):
    cosine, sine_table = rope_tables(positions, HD)
    full_shape = rotated_query_gradient.shape
    cotangent = rotated_query_gradient.astype(jnp.float32) * valid.astype(jnp.float32)[None, :, :, None]
    cotangent = cotangent.reshape(full_shape[:3] + (full_shape[3] // HD, HD // 2, 2))
    cosine = cosine[None, :, :, None, :]
    sine_table = sine_table[None, :, :, None, :]
    even_part = cosine * cotangent[..., 0] + sine_table * cotangent[..., 1]
    odd_part = cosine * cotangent[..., 1] - sine_table * cotangent[..., 0]
    unrotated = jnp.stack([even_part, odd_part], -1).reshape(full_shape)
    values = projections.astype(jnp.float32)
    inverse = lax.rsqrt(lax.optimization_barrier(jnp.mean(values * values, -1, keepdims=True)) + EPSILON)
    normed = values * inverse
    gain_part = lax.optimization_barrier(jnp.sum(unrotated * normed, axis=(1, 2)))
    scaled = unrotated * gains[:, None, None, :]
    projection_change = inverse * (scaled - normed * lax.optimization_barrier(jnp.mean(scaled * normed, -1, keepdims=True)))
    return (projection_change.astype(jnp.bfloat16), gain_part)

def adapter_partial_terms(projection_change, input_list, lowering_matrices, raising_matrices):
    down_terms = []
    up_terms = []
    for member in range(projection_change.shape[0]):
        reduced = jnp.dot(input_list, lowering_matrices[member].T, preferred_element_type=jnp.float32).astype(jnp.bfloat16)
        up_terms.append(jnp.dot(reduced.T, projection_change[member], preferred_element_type=jnp.float32))
        back_rank = jnp.dot(projection_change[member], raising_matrices[member].T, preferred_element_type=jnp.float32).astype(jnp.bfloat16)
        down_terms.append(jnp.dot(back_rank.T, input_list, preferred_element_type=jnp.float32))
    return (jnp.stack(down_terms), jnp.stack(up_terms))

def reference(projections, rotated_query_gradient, gains, adapter_lowering, adapter_raising, activations, positions, valid):
    count = jnp.sum(valid.astype(jnp.float32))
    factor = SAMPLES * LEN / count

    def one_sample(items):
        proj_one, grad_one, pos_one, valid_one, single_input = items
        projection_change, gain_part = norm_backward(proj_one[:, None], grad_one[:, None], gains, pos_one[:, None], valid_one[None])
        lowering_portion, raising_portion = adapter_partial_terms(projection_change[:, 0], single_input, adapter_lowering, adapter_raising)
        return (lowering_portion, raising_portion, gain_part)
    down_all, up_all, gain_all = lax.map(one_sample, (jnp.moveaxis(projections, 1, 0), jnp.moveaxis(rotated_query_gradient, 1, 0), jnp.moveaxis(positions, 1, 0), valid, activations))
    return (factor * lax.optimization_barrier(jnp.sum(down_all, 0)), factor * lax.optimization_barrier(jnp.sum(up_all, 0)), factor * lax.optimization_barrier(jnp.sum(gain_all, 0)))
```

```python
import functools
from types import SimpleNamespace

import jax
import jax.numpy as jnp
import numpy as np
from jax import lax
from jax.experimental import pallas as pl
from jax.experimental.pallas import tpu as pltpu
from jax.sharding import PartitionSpec as P

HD = 128
EPSILON = 1e-06
LANES = 128
BF = jnp.bfloat16
F32 = jnp.float32
MESH = pl.DeviceIdType.MESH
NT = (((1,), (1,)), ((), ()))


def group_counts():
    one_sixth = HD // 6
    return (HD // 2 - 2 * one_sixth, one_sixth, one_sixth)


def lane_frequencies():
    pieces = []
    for n in group_counts():
        pieces.append(np.float32(10000.0) ** (-np.arange(n, dtype=np.float32) / np.float32(n)))
    return np.repeat(np.concatenate(pieces).astype(np.float32), 2)[None]


def kernel(cfg, tree, *refs):
    inputs, outputs, scratch = jax.tree.unflatten(tree, refs)
    m = SimpleNamespace(**inputs, **outputs, **scratch)
    S, D, T, F, W = cfg.S, cfg.D, cfg.T, cfg.F, cfg.W
    R, RP, M, QF, KD = cfg.R, cfg.RP, cfg.M, cfg.QF, cfg.KD
    pieces = cfg.pieces
    K = S // 2
    T2 = 2 * T
    ranks = D * R
    groups = F // LANES
    hw = 256 if F % 256 == 0 else 128
    pow2 = K & (K - 1) == 0
    d = lax.axis_index("dp")
    s = lax.axis_index("seq")
    c = lax.rem(s, 2)
    chip = s // 2
    sib = s + 1 - 2 * c

    def to(j):
        if j == 0:
            return chip
        if not pow2:
            return lax.rem(chip + j, K)
        k, bit = chip, 1
        while bit < K:
            if j & bit:
                k = k + bit * (1 - 2 * lax.rem(chip // bit, 2))
            bit *= 2
        return k

    def slot(j):
        return j if pow2 else (K - j) % K

    chips = [to(j) for j in range(K)]

    def frm(j):
        return chips[slot(j)]

    def cols(start, width):
        return pl.ds(pl.multiple_of(start, LANES), width)

    def rows(core):
        return pl.ds(pl.multiple_of(core * T, T), T)

    def copy(src, dst, ss, rs, dp, seq):
        return pltpu.make_async_remote_copy(
            src_ref=src, dst_ref=dst, send_sem=ss, recv_sem=rs,
            device_id=(dp, seq), device_id_type=MESH,
        )

    def other(cc):
        return c if cc == 0 else 1 - c

    peers = [(j, cc) for j in range(K) for cc in range(2) if (j, cc) != (0, 0)]

    barrier = pltpu.get_barrier_semaphore()
    for j, cc in peers:
        pl.semaphore_signal(barrier, inc=1, device_id=(d, 2 * chips[j] + other(cc)), device_id_type=MESH)
    for k in range(1, D):
        pl.semaphore_signal(barrier, inc=1, device_id=(lax.rem(d + k, D), s), device_id_type=MESH)

    def local(src, dst, i):
        return pltpu.make_async_copy(src, dst, m.local_sem.at[i])

    low_load = local(m.low_hbm, m.low, 0)
    rai_load = local(m.rai_hbm, m.rai, 1)
    pos_load = local(m.pos_hbm, m.pos.at[c], 2)
    valid_load = local(m.valid_hbm, m.valid.at[c], 3)
    freq_load = local(m.freq_hbm, m.freq, 4)
    gains_load = local(m.gains_hbm, m.gains, 5)
    cot_loads = [
        local(m.cot_hbm.at[chips[j]], m.cot.at[0] if j == 0 else m.cot_src.at[j - 1], 6 if j == 0 else 7)
        for j in range(K)
    ]
    proj_loads = [
        local(m.proj_hbm.at[:, cols((2 * k + c) * F, F)], m.p2.at[rows(c), pl.ds(k * F, F)], 8)
        for k in range(K)
    ]
    act_loads = [
        local(m.act_hbm.at[:, cols((2 * k + c) * W, W)], m.a2.at[rows(c), pl.ds(k * W, W)], 9)
        for k in range(KD)
    ]
    low_load.start()
    rai_load.start()
    for j in range(1, K):
        cot_loads[j].start()
    pos_load.start()
    valid_load.start()
    freq_load.start()
    gains_load.start()
    cot_loads[0].start()
    for load in proj_loads + act_loads:
        load.start()

    fold, packed = m.fold, m.packed
    if packed.shape[1] > K * R or KD < K:
        fold[...] = jnp.zeros_like(fold)
    if KD < K:
        m.a2[:, KD * W:] = jnp.zeros((T2, (K - KD) * W), BF)
    low_load.wait()
    rai_load.wait()
    for q in range(K):
        if q < KD:
            fold[q * R:(q + 1) * R, 0:W] = m.low[:, cols((2 * q + c) * W, W)].astype(F32)
        fold[q * R:(q + 1) * R, W:W + F] = m.rai[:, cols((2 * q + c) * F, F)].astype(F32)
    packed[d] = fold[...].astype(BF)
    local(m.cot_hbm.at[0:K - 1], m.cot_src, 7).wait()

    def cot_copy(j, r):
        part = pl.ds(r * T, T)
        return copy(m.cot_src.at[j - 1, part], m.cot.at[j, part],
                    m.cot_s, m.cot_r.at[j, r], d, 2 * chips[j] + c)

    def adapt_copy(peer, place):
        return copy(packed.at[place], packed.at[place], m.ad_s, m.ad_r, peer, s)

    def sib_copy(src, dst, i):
        return copy(src, dst, m.sib_s.at[i], m.sib_r.at[i], d, sib)

    def pos_copy(core):
        return sib_copy(m.pos_hbm, m.pos.at[core], 0)

    def valid_copy(core):
        return sib_copy(m.valid_hbm, m.valid.at[core], 1)

    def proj_copy(k, core):
        return sib_copy(m.proj_hbm.at[:, cols((2 * k + 1 - c) * F, F)],
                        m.p2.at[rows(core), pl.ds(k * F, F)], 6)

    def act_copy(k, core):
        return sib_copy(m.act_hbm.at[:, cols((2 * k + 1 - c) * W, W)],
                        m.a2.at[rows(core), pl.ds(k * W, W)], 7)

    def xch_copy(send, recv, i):
        return sib_copy(send, recv, i)

    sq_copy = xch_copy(m.sq_send, m.sq_recv, 2)
    red_copy = xch_copy(m.red_send, m.red_recv, 3)
    dot_copy = xch_copy(m.dot_send, m.dot_recv, 4)
    back_copy = xch_copy(m.back_send, m.back_recv, 5)

    near = [j for j in range(1, K) if pow2 and j & (j - 1) == 0]
    far = [j for j in range(1, K) if j not in near]
    order = [(j, r) for r in range(2) for j in near] + [(j, r) for j in far for r in range(2)]

    pl.semaphore_wait(barrier, S + D - 2)
    for j, r in order:
        cot_copy(j, r).start()
    for k in range(1, D):
        adapt_copy(lax.rem(d + k, D), d).start()
    pos_copy(c).start()
    valid_copy(c).start()
    for k in range(K):
        proj_copy(k, c).start()
    for k in range(KD):
        act_copy(k, c).start()

    row_i = lax.broadcasted_iota(jnp.int32, (hw, hw), 0)
    col_i = lax.broadcasted_iota(jnp.int32, (hw, hw), 1)
    even = lax.rem(col_i, 2) == 0
    m.swap[...] = jnp.where(
        even & (row_i == col_i + 1), 1.0, jnp.where(jnp.logical_not(even) & (row_i == col_i - 1), -1.0, 0.0)
    ).astype(BF)

    pos_load.wait()
    valid_load.wait()
    freq_load.wait()
    gains_load.wait()
    pos_copy(1 - c).wait_recv()
    valid_copy(1 - c).wait_recv()
    n0, n1, _ = group_counts()
    lane = lax.broadcasted_iota(jnp.int32, (T, LANES), 1)

    def column(row):
        return jnp.broadcast_to(row.astype(F32), (LANES, T)).T

    count = jnp.zeros((1, 1), F32)
    for h in range(2):
        index = jnp.where(
            lane < 2 * n0, column(m.pos[h, 0]),
            jnp.where(lane < 2 * (n0 + n1), column(m.pos[h, 1]), column(m.pos[h, 2])),
        )
        angle = index * m.freq[...]
        ok = column(m.valid[h])
        m.cos[h * T:(h + 1) * T, :] = jnp.cos(angle) * ok
        m.sin[h * T:(h + 1) * T, :] = jnp.sin(angle) * ok
        count += jnp.sum(m.valid[h].astype(F32), axis=1, keepdims=True)
    m.small_send[...] = jnp.broadcast_to(count[:, :, None], m.small_send.shape)

    proj_all = m.proj_hbm.at[:, 0:K * F]
    local(proj_all, m.p2.at[rows(c)], 8).wait()
    sib_proj = sib_copy(proj_all, m.p2.at[rows(1 - c)], 6)
    sib_proj.wait_recv()
    square = jnp.zeros((T2, LANES), F32)
    for i in range(K * groups):
        v = m.p2[:, i * LANES:(i + 1) * LANES].astype(F32)
        square += v * v
    m.sq_send[...] = square
    sq_copy.start()
    m.dot_send[...] = jnp.zeros_like(m.dot_send)
    cot_loads[0].wait()
    sq_copy.wait_recv()
    square = m.sq_send[...] + m.sq_recv[...]
    inverse = lax.rsqrt(jnp.sum(square, axis=1, keepdims=True) / QF + EPSILON)
    m.inv[...] = jnp.broadcast_to(inverse, (T2, LANES))

    def wide(x):
        return jnp.concatenate([x] * (hw // LANES), axis=1) if hw > LANES else x

    def chunk(j, r):
        k = frm(j)
        part = slice(r * T, (r + 1) * T)
        inv = wide(m.inv[part])
        cw, sw = wide(m.cos[part]), wide(m.sin[part])
        for i in range(F // hw):
            x = m.cot[j, part, i * hw:(i + 1) * hw]
            xs = jnp.dot(x, m.swap[...], preferred_element_type=F32)
            un = cw * x.astype(F32) + sw * xs
            prod = un * (m.p2[part, cols(k * F + i * hw, hw)].astype(F32) * inv)
            g = jnp.sum(prod, axis=0, keepdims=True)
            for t in range(hw // LANES):
                n = i * (hw // LANES) + t
                piece = g[:, t * LANES:(t + 1) * LANES]
                if r > 0:
                    piece += m.small_send[j, n:n + 1, :]
                m.small_send[j, n:n + 1, :] = piece
            gn = m.gains[:, cols((2 * k + c) * F + i * hw, hw)]
            m.scaled[j, part, i * hw:(i + 1) * hw] = un * gn
            pg = prod * gn
            acc = pg[:, :LANES]
            for t in range(1, hw // LANES):
                acc += pg[:, t * LANES:(t + 1) * LANES]
            m.dot_send[part] += acc

    chunk(0, 0)
    chunk(0, 1)
    cut = len(order) - 1
    for j, r in order[:cut]:
        cot_copy(j, r).wait_recv()
        chunk(j, r)

    adapt_all = copy(packed.at[0:D - 1], packed.at[0:D - 1], m.ad_s, m.ad_r, d, sib)
    adapt_all.wait_recv()
    adaptf, adapt = m.adaptf, m.adapt
    for e in range(D):
        fold[...] = packed[e].astype(F32)
        for q in range(K):
            adaptf[q, e * R:(e + 1) * R, :] = fold[q * R:(q + 1) * R, :]
    for q in range(K):
        adapt[q] = adaptf[q].astype(BF)
    act_all = m.act_hbm.at[:, 0:KD * W]
    local(act_all, m.a2.at[rows(c), 0:KD * W], 9).wait()
    sib_act = sib_copy(act_all, m.a2.at[rows(1 - c), 0:KD * W], 7)
    sib_act.wait_recv()
    red = jnp.zeros((ranks, T2), F32)
    for k in range(KD):
        red += lax.dot_general(adapt[k, :, 0:W], m.a2[:, k * W:(k + 1) * W], NT, preferred_element_type=F32)
    m.red_send[...] = red
    red_copy.start()

    for j, r in order[cut:]:
        cot_copy(j, r).wait_recv()
        chunk(j, r)

    dot_copy.start()

    def small_copy(j):
        return copy(m.small_send.at[slot(j)], m.small_recv.at[j - 1], m.sm_s, m.sm_r, d, 2 * chips[j] + c)

    for j in range(1, K):
        small_copy(j).start()
    red_copy.wait_recv()
    redt = (m.red_send[...] + m.red_recv[...]).astype(BF)
    m.redt[...] = redt
    dot_copy.wait_recv()
    mean = jnp.sum(m.dot_send[...] + m.dot_recv[...], axis=1, keepdims=True) / QF
    inv = m.inv[...]
    m.coef[...] = inv * inv * jnp.broadcast_to(mean, (T2, LANES))

    def rs_copy(i, j):
        return copy(m.rs_send[i].at[j - 1], m.rs_recv[i].at[j - 1],
                    m.rs_s.at[i], m.rs_r.at[i], d, 2 * chips[j] + c)

    def whole(src, dst, ss, rs):
        return copy(src, dst, ss, rs, d, sib)

    back = jnp.zeros((ranks, T2), F32)
    for js in (near, far + [0]):
        for j in js:
            k = chips[j]
            inv, coef = wide(m.inv[...]), wide(m.coef[...])
            for i in range(F // hw):
                part = slice(i * hw, (i + 1) * hw)
                p = m.p2[:, cols(k * F + i * hw, hw)].astype(F32)
                delta = (inv * m.scaled[slot(j), :, part] - coef * p).astype(BF)
                raising = adapt[k, :, W + i * hw:W + (i + 1) * hw]
                back += lax.dot_general(raising, delta, NT, preferred_element_type=F32)
                term = jnp.dot(m.redt[...], delta, preferred_element_type=F32)
                if j == 0:
                    m.own[0][:, part] = term
                else:
                    m.rs_send[0][j - 1, :, part] = term.astype(BF)
        for j in js:
            if j > 0:
                rs_copy(0, j).start()
    m.back_send[...] = back
    back_copy.start()
    back_copy.wait_recv()
    m.backt[...] = (m.back_send[...] + m.back_recv[...]).astype(BF)

    for i, (kind, off, width) in enumerate(pieces):
        if kind == "u":
            continue
        for j in list(range(1, K)) + [0]:
            term = jnp.dot(m.backt[...], m.a2[:, cols(chips[j] * W + off, width)], preferred_element_type=F32)
            if j == 0:
                m.own[i][...] = term
            else:
                m.rs_send[i][j - 1] = term.astype(BF)
        for j in range(1, K):
            rs_copy(i, j).start()

    small = m.small_send[0]
    small_all = whole(m.small_recv, m.small_recv, m.sm_s, m.sm_r)
    small_all.wait_recv()
    for j in range(1, K):
        small += m.small_recv[j - 1]
    m.small_dp[...] = small

    def small_dp_copy(k):
        return copy(m.small_dp, m.small_dp_recv.at[k - 1], m.smd_s, m.smd_r, lax.rem(d + k, D), s)

    for k in range(1, D):
        small_dp_copy(k).start()

    def dp_copy(i, k):
        return copy(m.dp_send[i].at[lax.rem(d + k, D)], m.dp_recv[i].at[k - 1],
                    m.dp_s.at[i], m.dp_r.at[i], lax.rem(d + k, D), s)

    def dp_stage(i):
        total = m.own[i][...]
        whole(m.rs_send[i], m.rs_recv[i], m.rs_s.at[i], m.rs_r.at[i]).wait_recv()
        for j in range(1, K):
            total += m.rs_recv[i][j - 1].astype(F32)
        tot = m.tot[i]
        tot[0:ranks, :] = total
        for e in range(D):
            block = tot[e * R:e * R + RP, :]
            m.dp_f[i][e] = block
            m.dp_send[i][e] = block.astype(BF)
        for k in range(1, D):
            dp_copy(i, k).start()

    def ag_copy(i, j, cc):
        return copy(m.fin[i], m.ag[i].at[2 * j + cc - 1], m.ag_s.at[i], m.ag_r.at[i],
                    d, 2 * chips[j] + other(cc))

    def put(i, q, value):
        kind, off, width = pieces[i]
        out, base = (m.up_out, q * F) if kind == "u" else (m.down_out, q * W + off)

        def store():
            where = cols(base, width)
            for r in range(R):
                out[r, :, where] = value[r:r + 1]

        if kind == "d" and S * W != M:
            pl.when(base + width <= M)(store)
        else:
            store()

    def dp_all(i):
        return whole(m.dp_send[i].at[0:D - 1], m.dp_recv[i], m.dp_s.at[i], m.dp_r.at[i])

    def ag_all(i):
        return whole(m.ag[i], m.ag[i], m.ag_s.at[i], m.ag_r.at[i])

    def gather(i, factor):
        total = m.dp_f[i][d]
        dp_all(i).wait_recv()
        for k in range(1, D):
            total += m.dp_recv[i][k - 1].astype(F32)
        fin = (total * factor).astype(BF)
        m.fin[i][...] = fin
        for j, cc in peers:
            ag_copy(i, j, cc).start()
        put(i, s, fin.astype(F32))

    for i in range(len(pieces)):
        dp_stage(i)

    small = m.small_dp[...]
    small_dp_all = whole(m.small_dp_recv, m.small_dp_recv, m.smd_s, m.smd_r)
    small_dp_all.wait_recv()
    for k in range(1, D):
        small += m.small_dp_recv[k - 1]
    factor = F32(cfg.tokens) / small[groups:groups + 1, 0:1]
    m.small_fin[...] = small * factor

    def small_ag_copy(j, cc):
        return copy(m.small_fin, m.small_ag.at[2 * j + cc - 1], m.sma_s, m.sma_r,
                    d, 2 * chips[j] + other(cc))

    for j, cc in peers:
        small_ag_copy(j, cc).start()

    for i in range(len(pieces)):
        gather(i, factor)

    def put_gain(q, value):
        for n in range(groups):
            m.gain_out[:, cols(q * F + n * LANES, LANES)] = value[n:n + 1, :]

    put_gain(s, m.small_fin[...])
    small_ag_all = whole(m.small_ag, m.small_ag, m.sma_s, m.sma_r)
    small_ag_all.wait_recv()
    for j, cc in peers:
        put_gain(2 * frm(j) + other(cc), m.small_ag[2 * j + cc - 1])
    for i in range(len(pieces)):
        ag_all(i).wait_recv()
        for j, cc in peers:
            put(i, 2 * frm(j) + other(cc), m.ag[i][2 * j + cc - 1].astype(F32))

    pos_copy(c).wait_send()
    valid_copy(c).wait_send()
    whole(m.cot_src, m.cot_src, m.cot_s, m.cot_r.at[0, 0]).wait_send()
    for group in (sib_proj, sib_act, sq_copy, red_copy, dot_copy, back_copy,
                  adapt_all, small_all, small_dp_all, small_ag_all):
        group.wait_send()
    for i in range(len(pieces)):
        whole(m.rs_send[i], m.rs_recv[i], m.rs_s.at[i], m.rs_r.at[i]).wait_send()
        dp_all(i).wait_send()
        ag_all(i).wait_send()


def write_out(*refs):
    n = len(refs) // 2
    copies = [pltpu.make_async_copy(refs[i], refs[n + i], refs[2 * n].at[i]) for i in range(n)]
    for copy in copies:
        copy.start()
    for copy in copies:
        copy.wait()


def block_width(M, S):
    width = -(-M // (LANES * S)) * LANES
    while M % (2 * width):
        width += LANES
    return width


def shards(projections, rotated_query_gradient, gains, adapter_lowering, adapter_raising,
           activations, positions, valid):
    D, S = lax.axis_size("dp"), lax.axis_size("seq")
    T, QF = projections.shape[2:]
    F = rotated_query_gradient.shape[3]
    R, M = adapter_lowering.shape[1:]
    W = block_width(M, S)
    KD = M // (2 * W)
    RP = -(-R // 16) * 16
    K = S // 2
    T2 = 2 * T
    ranks = D * R
    folded = -(-K * R // 16) * 16
    first = -(-W // (2 * LANES)) * LANES
    pieces = [("u", 0, F), ("d", 0, first)] + ([("d", first, W - first)] if W > first else [])
    cfg = SimpleNamespace(S=S, D=D, T=T, F=F, W=W, R=R, RP=RP, M=M, QF=QF, KD=KD, tokens=D * S * T, pieces=pieces)

    hw = 256 if F % 256 == 0 else 128
    small_rows = -(-(F // LANES + 1) // 8) * 8
    vmem = pltpu.VMEM
    dma = pltpu.SemaphoreType.DMA
    scratch = dict(
        p2=vmem((T2, K * F), BF),
        a2=vmem((T2, K * W), BF),
        cot=vmem((K, T2, F), BF),
        cot_src=vmem((K - 1, T2, F), BF),
        low=vmem((R, M), BF),
        rai=vmem((R, QF), BF),
        pos=vmem((2, 3, 1, T), jnp.int32),
        valid=vmem((2, 1, T), jnp.int32),
        freq=vmem((1, LANES), F32),
        gains=vmem((1, QF), F32),
        swap=vmem((hw, hw), BF),
        fold=vmem((folded, W + F), F32),
        packed=vmem((D, folded, W + F), BF),
        adaptf=vmem((K, ranks, W + F), F32),
        adapt=vmem((K, ranks, W + F), BF),
        scaled=vmem((K, T2, F), F32),
        cos=vmem((T2, LANES), F32),
        sin=vmem((T2, LANES), F32),
        inv=vmem((T2, LANES), F32),
        coef=vmem((T2, LANES), F32),
        sq_send=vmem((T2, LANES), F32),
        sq_recv=vmem((T2, LANES), F32),
        dot_send=vmem((T2, LANES), F32),
        dot_recv=vmem((T2, LANES), F32),
        red_send=vmem((ranks, T2), F32),
        red_recv=vmem((ranks, T2), F32),
        back_send=vmem((ranks, T2), F32),
        back_recv=vmem((ranks, T2), F32),
        redt=vmem((ranks, T2), BF),
        backt=vmem((ranks, T2), BF),
        small_send=vmem((K, small_rows, LANES), F32),
        small_recv=vmem((K - 1, small_rows, LANES), F32),
        small_dp=vmem((small_rows, LANES), F32),
        small_dp_recv=vmem((D - 1, small_rows, LANES), F32),
        small_fin=vmem((small_rows, LANES), F32),
        small_ag=vmem((S - 1, small_rows, LANES), F32),
    )
    for kind, off, width in pieces:
        for name, value in dict(
            rs_send=vmem((K - 1, ranks, width), BF),
            rs_recv=vmem((K - 1, ranks, width), BF),
            own=vmem((ranks, width), F32),
            tot=vmem((ranks + RP, width), F32),
            dp_f=vmem((D, RP, width), F32),
            dp_send=vmem((D, RP, width), BF),
            dp_recv=vmem((D - 1, RP, width), BF),
            fin=vmem((RP, width), BF),
            ag=vmem((S - 1, RP, width), BF),
        ).items():
            scratch.setdefault(name, []).append(value)
    n = len(pieces)
    sems = dict(
        local_sem=(10,), cot_s=(), cot_r=(K, 2), ad_s=(), ad_r=(), sib_s=(8,), sib_r=(8,),
        sm_s=(), sm_r=(), smd_s=(), smd_r=(), sma_s=(), sma_r=(),
        rs_s=(n,), rs_r=(n,), dp_s=(n,), dp_r=(n,), ag_s=(n,), ag_r=(n,),
    )
    scratch.update({name: dma(shape) if shape else dma for name, shape in sems.items()})
    hbm = pl.BlockSpec(memory_space=pltpu.HBM)
    inputs = dict(
        proj_hbm=projections.reshape(T, QF),
        cot_hbm=rotated_query_gradient.reshape(K, T2, F),
        act_hbm=activations.reshape(T, M),
        low_hbm=adapter_lowering[0],
        rai_hbm=adapter_raising[0],
        gains_hbm=gains,
        freq_hbm=jnp.asarray(lane_frequencies()),
        pos_hbm=positions,
        valid_hbm=valid.reshape(1, T),
    )
    outputs = dict(
        down_out=jax.ShapeDtypeStruct((R, 1, M), F32),
        up_out=jax.ShapeDtypeStruct((R, 1, QF), F32),
        gain_out=jax.ShapeDtypeStruct((1, QF), F32),
    )
    leaves, tree = jax.tree.flatten([inputs, outputs, scratch])
    count = len(inputs) + len(outputs)
    results = pl.pallas_call(
        functools.partial(kernel, cfg, tree),
        out_shape=leaves[len(inputs):count],
        in_specs=[hbm] * len(inputs),
        out_specs=[pl.BlockSpec(memory_space=vmem)] * len(outputs),
        scratch_shapes=leaves[count:],
        compiler_params=pltpu.CompilerParams(
            collective_id=0, has_side_effects=True, vmem_limit_bytes=40 * 1024 * 1024
        ),
    )(*[pltpu.with_memory_space_constraint(x, pltpu.HBM) for x in leaves[:len(inputs)]])
    results = pl.pallas_call(
        write_out,
        out_shape=leaves[len(inputs):count],
        in_specs=[pl.BlockSpec(memory_space=vmem)] * len(outputs),
        out_specs=[hbm] * len(outputs),
        scratch_shapes=[dma((len(outputs),))],
        compiler_params=pltpu.CompilerParams(vmem_limit_bytes=1024 * 1024),
    )(*results)
    down, gain, up = results
    return down.reshape(1, R, M), up.reshape(1, R, QF), gain


def solution(mesh):
    in_specs = (
        P(None, "dp", "seq", None),
        P(None, "dp", None, "seq"),
        P(),
        P(None, "dp", None),
        P(None, "dp", None),
        P("dp", "seq", None),
        P(None, "dp", "seq"),
        P("dp", "seq"),
    )
    out_specs = (P(None, "dp", None), P(None, "dp", None), P())
    return jax.shard_map(shards, mesh=mesh, in_specs=in_specs, out_specs=out_specs, check_vma=False)
```

```python
import functools
from types import SimpleNamespace

import jax
import jax.numpy as jnp
import numpy as np
from jax import lax
from jax.experimental import pallas as pl
from jax.experimental.pallas import tpu as pltpu
from jax.sharding import PartitionSpec as P

HD = 128
EPSILON = 1e-06
LANES = 128
BF = jnp.bfloat16
F32 = jnp.float32
MESH = pl.DeviceIdType.MESH
NT = (((1,), (1,)), ((), ()))


def group_counts():
    one_sixth = HD // 6
    return (HD // 2 - 2 * one_sixth, one_sixth, one_sixth)


def lane_frequencies():
    pieces = []
    for n in group_counts():
        pieces.append(np.float32(10000.0) ** (-np.arange(n, dtype=np.float32) / np.float32(n)))
    return np.repeat(np.concatenate(pieces).astype(np.float32), 2)[None]


def kernel(cfg, tree, *refs):
    inputs, outputs, scratch = jax.tree.unflatten(tree, refs)
    m = SimpleNamespace(**inputs, **outputs, **scratch)
    S, D, T, F, W = cfg.S, cfg.D, cfg.T, cfg.F, cfg.W
    R, RP, M, QF, KD, Z = cfg.R, cfg.RP, cfg.M, cfg.QF, cfg.KD, cfg.Z
    pieces = cfg.pieces
    K = S // 2
    T2 = 2 * T
    ranks = D * R
    groups = F // LANES
    hw = 256 if F % 256 == 0 else 128
    pow2 = K & (K - 1) == 0
    d = lax.axis_index("dp")
    s = lax.axis_index("seq")
    c = lax.rem(s, 2)
    chip = s // 2
    sib = s + 1 - 2 * c

    def to(j):
        if j == 0:
            return chip
        if not pow2:
            return lax.rem(chip + j, K)
        k, bit = chip, 1
        while bit < K:
            if j & bit:
                k = k + bit * (1 - 2 * lax.rem(chip // bit, 2))
            bit *= 2
        return k

    def slot(j):
        return j if pow2 else (K - j) % K

    chips = [to(j) for j in range(K)]

    def frm(j):
        return chips[slot(j)]

    def cols(start, width):
        return pl.ds(pl.multiple_of(start, LANES), width)

    def rows(core):
        return pl.ds(pl.multiple_of(core * T, T), T)

    def copy(src, dst, ss, rs, dp, seq):
        return pltpu.make_async_remote_copy(
            src_ref=src, dst_ref=dst, send_sem=ss, recv_sem=rs,
            device_id=(dp, seq), device_id_type=MESH,
        )

    def other(cc):
        return c if cc == 0 else 1 - c

    peers = [(j, cc) for j in range(K) for cc in range(2) if (j, cc) != (0, 0)]

    barrier = pltpu.get_barrier_semaphore()
    for j, cc in peers:
        pl.semaphore_signal(barrier, inc=1, device_id=(d, 2 * chips[j] + other(cc)), device_id_type=MESH)
    for k in range(1, D):
        pl.semaphore_signal(barrier, inc=1, device_id=(lax.rem(d + k, D), s), device_id_type=MESH)

    def local(src, dst, i):
        return pltpu.make_async_copy(src, dst, m.local_sem.at[i])

    low_load = local(m.low_hbm, m.low, 0)
    rai_load = local(m.rai_hbm, m.rai, 1)
    pos_load = local(m.pos_hbm, m.pos.at[c], 2)
    valid_load = local(m.valid_hbm, m.valid.at[c], 3)
    freq_load = local(m.freq_hbm, m.freq, 4)
    gains_load = local(m.gains_hbm, m.gains, 5)
    cot_loads = [
        local(m.cot_hbm.at[chips[j]], m.cot.at[0] if j == 0 else m.cot_src.at[j - 1], 10 + j)
        for j in range(K)
    ]
    proj_loads = [
        local(m.proj_hbm.at[:, cols((2 * k + c) * F, F)], m.p2.at[rows(c), pl.ds(k * F, F)], 8)
        for k in range(K)
    ]
    act_loads = [
        local(m.act_hbm.at[:, cols((2 * k + c) * W, W)], m.a2.at[rows(c), pl.ds(k * W, W)], 9)
        for k in range(KD)
    ]
    for j in range(1, K):
        cot_loads[j].start()
    low_load.start()
    rai_load.start()
    pos_load.start()
    valid_load.start()
    freq_load.start()
    gains_load.start()
    cot_loads[0].start()
    for load in proj_loads + act_loads:
        load.start()

    def cot_copy(j, r):
        part = pl.ds(r * T, T)
        return copy(m.cot_src.at[j - 1, part], m.cot.at[j, part],
                    m.cot_s, m.cot_r.at[j, r], d, 2 * chips[j] + c)

    def raise_copy(k):
        return copy(m.packed_r.at[d], m.packed_r.at[d], m.ar_s, m.ar_r, lax.rem(d + k, D), s)

    def lower_copy(k):
        return copy(m.packed_l.at[d], m.packed_l.at[d], m.al_s, m.al_r, lax.rem(d + k, D), s)

    def sib_copy(src, dst, i):
        return copy(src, dst, m.sib_s.at[i], m.sib_r.at[i], d, sib)

    def pos_copy(core):
        return sib_copy(m.pos_hbm, m.pos.at[core], 0)

    def valid_copy(core):
        return sib_copy(m.valid_hbm, m.valid.at[core], 1)

    def proj_copy(k, core):
        return sib_copy(m.proj_hbm.at[:, cols((2 * k + 1 - c) * F, F)],
                        m.p2.at[rows(core), pl.ds(k * F, F)], 6)

    def act_copy(k, core):
        return sib_copy(m.act_hbm.at[:, cols((2 * k + 1 - c) * W, W)],
                        m.a2.at[rows(core), pl.ds(k * W, W)], 7)

    def xch_copy(send, recv, i):
        return sib_copy(send, recv, i)

    sq_copy = xch_copy(m.sq_send, m.sq_recv, 2)
    red_copy = xch_copy(m.red_send, m.red_recv, 3)
    base_copy = xch_copy(m.base_send, m.base_recv, 4)
    back_copy = xch_copy(m.back_send, m.back_recv, 5)

    near = [j for j in range(1, K) if pow2 and j & (j - 1) == 0]
    far = [j for j in range(1, K) if j not in near]
    order = [(j, r) for r in range(2) for j in near] + [(j, r) for j in far for r in range(2)]

    pl.semaphore_wait(barrier, S + D - 2)
    pos_copy(c).start()
    valid_copy(c).start()
    for j in near:
        cot_loads[j].wait()
        cot_copy(j, 0).start()
    for j in near:
        cot_copy(j, 1).start()
    for j in far:
        cot_loads[j].wait()

    def far_sends():
        for j in far:
            for r in range(2):
                cot_copy(j, r).start()

    pl.when(c == 0)(far_sends)
    fold = m.fold
    if fold.shape[0] > K * R or KD < K:
        fold[...] = jnp.zeros_like(fold)
    if KD < K:
        m.a2[:, KD * W:] = jnp.zeros((T2, (K - KD) * W), BF)
    low_load.wait()
    rai_load.wait()
    for q in range(K):
        if q < KD:
            fold[q * R:(q + 1) * R, 0:W] = m.low[:, cols((2 * q + c) * W, W)].astype(F32)
        fold[q * R:(q + 1) * R, W:W + F] = m.rai[:, cols((2 * q + c) * F, F)].astype(F32)
    m.packed_r[d] = fold[:, W:].astype(BF)
    m.packed_l[d] = fold[:, :W].astype(BF)

    for k in range(1, D):
        raise_copy(k).start()
    for k in range(1, D):
        lower_copy(k).start()
    for k in range(K):
        proj_copy(k, c).start()
    for k in range(KD):
        act_copy(k, c).start()

    row_i = lax.broadcasted_iota(jnp.int32, (hw, hw), 0)
    col_i = lax.broadcasted_iota(jnp.int32, (hw, hw), 1)
    even = lax.rem(col_i, 2) == 0
    m.swap[...] = jnp.where(
        even & (row_i == col_i + 1), 1.0, jnp.where(jnp.logical_not(even) & (row_i == col_i - 1), -1.0, 0.0)
    ).astype(BF)

    pos_load.wait()
    valid_load.wait()
    freq_load.wait()
    gains_load.wait()
    pos_copy(1 - c).wait_recv()
    valid_copy(1 - c).wait_recv()
    n0, n1, _ = group_counts()
    lane = lax.broadcasted_iota(jnp.int32, (T, LANES), 1)

    def column(row):
        return jnp.broadcast_to(row.astype(F32), (LANES, T)).T

    count = jnp.zeros((1, 1), F32)
    for h in range(2):
        index = jnp.where(
            lane < 2 * n0, column(m.pos[h, 0]),
            jnp.where(lane < 2 * (n0 + n1), column(m.pos[h, 1]), column(m.pos[h, 2])),
        )
        angle = index * m.freq[...]
        ok = column(m.valid[h])
        m.cos[h * T:(h + 1) * T, :] = jnp.cos(angle) * ok
        m.sin[h * T:(h + 1) * T, :] = jnp.sin(angle) * ok
        count += jnp.sum(m.valid[h].astype(F32), axis=1, keepdims=True)
    m.small_send[...] = jnp.broadcast_to(count[:, :, None], m.small_send.shape)

    proj_all = m.proj_hbm.at[:, 0:K * F]
    local(proj_all, m.p2.at[rows(c)], 8).wait()
    sib_proj = sib_copy(proj_all, m.p2.at[rows(1 - c)], 6)
    sib_proj.wait_recv()
    square = jnp.zeros((T2, LANES), F32)
    for i in range(K * groups):
        v = m.p2[:, i * LANES:(i + 1) * LANES].astype(F32)
        square += v * v
    m.sq_send[...] = square
    sq_copy.start()
    m.dot[...] = jnp.zeros_like(m.dot)
    cot_loads[0].wait()
    sq_copy.wait_recv()
    square = m.sq_send[...] + m.sq_recv[...]
    inverse = lax.rsqrt(jnp.sum(square, axis=1, keepdims=True) / QF + EPSILON)
    inverse = jnp.broadcast_to(inverse, (T2, LANES))
    m.inv[...] = inverse
    m.inv_row[...] = inverse.T[0:1, :]

    def wide(x):
        return jnp.concatenate([x] * (hw // LANES), axis=1) if hw > LANES else x

    def chunk(j, r):
        k = frm(j)
        part = slice(r * T, (r + 1) * T)
        inv = wide(m.inv[part])
        cw, sw = wide(m.cos[part]), wide(m.sin[part])
        for i in range(F // hw):
            x = m.cot[j, part, i * hw:(i + 1) * hw]
            xs = jnp.dot(x, m.swap[...], preferred_element_type=F32)
            un = cw * x.astype(F32) + sw * xs
            prod = un * (m.p2[part, cols(k * F + i * hw, hw)].astype(F32) * inv)
            g = jnp.sum(prod, axis=0, keepdims=True)
            for t in range(hw // LANES):
                n = i * (hw // LANES) + t
                piece = g[:, t * LANES:(t + 1) * LANES]
                if r > 0:
                    piece += m.small_send[j, n:n + 1, :]
                m.small_send[j, n:n + 1, :] = piece
            gn = m.gains[:, cols((2 * k + c) * F + i * hw, hw)]
            m.scaled[j, part, i * hw:(i + 1) * hw] = un * gn * inv
            pg = prod * gn
            acc = pg[:, :LANES]
            for t in range(1, hw // LANES):
                acc += pg[:, t * LANES:(t + 1) * LANES]
            m.dot[part] += acc

    def whole(src, dst, ss, rs):
        return copy(src, dst, ss, rs, d, sib)

    def unfold(packed, adaptf, adapt):
        for e in range(D):
            fold[:, :packed.shape[2]] = packed[e].astype(F32)
            for q in range(K):
                adaptf[q, e * R:(e + 1) * R, :] = fold[q * R:(q + 1) * R, :packed.shape[2]]
        for q in range(K):
            adapt[q] = adaptf[q].astype(BF)

    def back_part(j, r):
        part = slice(r * T, (r + 1) * T)
        raising = m.adapt_r[frm(j)]
        value = m.scaled[j, part, :]
        high = value.astype(BF)
        low = (value - high.astype(F32)).astype(BF)
        term = lax.dot_general(raising, high, NT, preferred_element_type=F32)
        return term + lax.dot_general(raising, low, NT, preferred_element_type=F32)

    chunk(0, 0)
    chunk(0, 1)
    split = 2 * len(near)
    for (j, r), n in zip(order[:split], range(split)):
        cot_copy(j, r).wait_recv()
        if n == 2:
            pl.when(c == 1)(far_sends)
        chunk(j, r)
    raise_all = whole(m.packed_r.at[0:D - 1], m.packed_r.at[0:D - 1], m.ar_s, m.ar_r)
    raise_all.wait_recv()
    unfold(m.packed_r, m.adaptf_r, m.adapt_r)
    base = jnp.zeros((ranks, T2), F32)
    for k in range(K):
        base += lax.dot_general(m.adapt_r[k], m.p2[:, k * F:(k + 1) * F], NT, preferred_element_type=F32)
    m.base_send[...] = base
    base_copy.start()
    for r in range(2):
        total = jnp.zeros((ranks, T), F32)
        for j in [0] + near:
            total += back_part(j, r)
        m.back_send[0:ranks, r * T:(r + 1) * T] = total

    for j, r in order[split:-1]:
        cot_copy(j, r).wait_recv()
        chunk(j, r)
        m.back_send[0:ranks, r * T:(r + 1) * T] += back_part(j, r)
    lower_all = whole(m.packed_l.at[0:D - 1], m.packed_l.at[0:D - 1], m.al_s, m.al_r)
    lower_all.wait_recv()
    unfold(m.packed_l, m.adaptf_l, m.adapt_l)
    act_all = m.act_hbm.at[:, 0:KD * W]
    local(act_all, m.a2.at[rows(c), 0:KD * W], 9).wait()
    sib_act = sib_copy(act_all, m.a2.at[rows(1 - c), 0:KD * W], 7)
    sib_act.wait_recv()
    red = jnp.zeros((ranks, T2), F32)
    for k in range(KD):
        red += lax.dot_general(m.adapt_l[k], m.a2[:, k * W:(k + 1) * W], NT, preferred_element_type=F32)
    m.red_send[...] = red
    red_copy.start()
    base_copy.wait_recv()
    inv_row = m.inv_row[...]
    m.base[...] = (m.base_send[...] + m.base_recv[...]) * (inv_row * inv_row)

    for j, r in order[-1:]:
        cot_copy(j, r).wait_recv()
        chunk(j, r)
        m.back_send[0:ranks, r * T:(r + 1) * T] += back_part(j, r)
    dot_row = jnp.sum(m.dot[...].T, axis=0, keepdims=True)
    m.back_send[ranks:ranks + 8, :] = jnp.broadcast_to(dot_row, (8, T2))
    back_copy.start()

    def small_copy(j):
        return copy(m.small_send.at[slot(j)], m.small_recv.at[j - 1], m.sm_s, m.sm_r, d, 2 * chips[j] + c)

    for j in range(1, K):
        small_copy(j).start()
    red_copy.wait_recv()
    m.redt[...] = (m.red_send[...] + m.red_recv[...]).astype(BF)
    back_copy.wait_recv()
    back = m.back_send[...] + m.back_recv[...]
    mean_row = back[ranks:ranks + 1, :] / QF
    m.backt[...] = (back[0:ranks, :] - mean_row * m.base[...]).astype(BF)
    mean = jnp.broadcast_to(mean_row, (LANES, T2)).T
    inv = m.inv[...]
    m.coef[...] = inv * inv * mean

    def rs_copy(i, j):
        return copy(m.rs_send[i].at[j - 1], m.rs_recv[i].at[j - 1],
                    m.rs_s.at[i], m.rs_r.at[i], d, 2 * chips[j] + c)

    last = len(pieces) - 1
    for i, (kind, off, width) in enumerate(pieces[:last]):
        for j in list(range(1, K)) + [0]:
            term = jnp.dot(m.backt[...], m.a2[:, cols(chips[j] * W + off, width)], preferred_element_type=F32)
            if j == 0:
                m.own[i][...] = term
            else:
                m.rs_send[i][j - 1] = term.astype(BF)
        for j in range(1, K):
            rs_copy(i, j).start()

    for j in list(range(1, K)) + [0]:
        k = chips[j]
        coef = wide(m.coef[...])
        for i in range(F // hw):
            part = slice(i * hw, (i + 1) * hw)
            p = m.p2[:, cols(k * F + i * hw, hw)].astype(F32)
            delta = (m.scaled[slot(j), :, part] - coef * p).astype(BF)
            term = jnp.dot(m.redt[...], delta, preferred_element_type=F32)
            start = i * hw
            if start < Z:
                m.z_term[k, :, start:min(start + hw, Z)] = term[:, :min(hw, Z - start)]
            if start + hw > Z:
                rest = slice(max(start - Z, 0), start + hw - Z)
                term = term[:, hw - (rest.stop - rest.start):]
                if j == 0:
                    m.own[last][:, rest] = term
                else:
                    m.rs_send[last][j - 1, :, rest] = term.astype(BF)
    for j in range(1, K):
        rs_copy(last, j).start()

    def z_copy(k):
        return copy(m.z_send.at[lax.rem(d + k, D)], m.z_recv.at[k - 1], m.z_s, m.z_r, lax.rem(d + k, D), s)

    def z_share(j):
        return copy(m.z_ag.at[chip], m.z_ag.at[chip], m.zag_s, m.zag_r, d, 2 * chips[j] + c)

    if Z:
        for e in range(D):
            for k in range(K):
                m.z_f[e, k * R:(k + 1) * R, :] = m.z_term[k, e * R:(e + 1) * R, :]
            m.z_send[e] = m.z_f[e].astype(BF)
        for k in range(1, D):
            z_copy(k).start()
    small = m.small_send[0]
    small_all = whole(m.small_recv, m.small_recv, m.sm_s, m.sm_r)
    small_all.wait_recv()
    for j in range(1, K):
        small += m.small_recv[j - 1]
    m.small_dp[...] = small

    def small_dp_copy(k):
        return copy(m.small_dp, m.small_dp_recv.at[k - 1], m.smd_s, m.smd_r, lax.rem(d + k, D), s)

    for k in range(1, D):
        small_dp_copy(k).start()

    def dp_copy(i, k):
        return copy(m.dp_send[i].at[lax.rem(d + k, D)], m.dp_recv[i].at[k - 1],
                    m.dp_s.at[i], m.dp_r.at[i], lax.rem(d + k, D), s)

    def dp_stage(i):
        total = m.own[i][...]
        whole(m.rs_send[i], m.rs_recv[i], m.rs_s.at[i], m.rs_r.at[i]).wait_recv()
        for j in range(1, K):
            total += m.rs_recv[i][j - 1].astype(F32)
        tot = m.tot[i]
        tot[0:ranks, :] = total
        for e in range(D):
            block = tot[e * R:e * R + RP, :]
            m.dp_f[i][e] = block
            m.dp_send[i][e] = block.astype(BF)
        for k in range(1, D):
            dp_copy(i, k).start()

    def ag_copy(i, j, cc):
        return copy(m.fin[i], m.ag[i].at[2 * j + cc - 1], m.ag_s.at[i], m.ag_r.at[i],
                    d, 2 * chips[j] + other(cc))

    def put(i, q, value):
        kind, off, width = pieces[i]
        out, base = (m.up_out, q * F + off) if kind == "u" else (m.down_out, q * W + off)

        def store():
            where = cols(base, width)
            for r in range(R):
                out[r, :, where] = value[r:r + 1]

        if kind == "d" and S * W != M:
            pl.when(base + width <= M)(store)
        else:
            store()

    def dp_all(i):
        return whole(m.dp_send[i].at[0:D - 1], m.dp_recv[i], m.dp_s.at[i], m.dp_r.at[i])

    def ag_all(i):
        return whole(m.ag[i], m.ag[i], m.ag_s.at[i], m.ag_r.at[i])

    def gather(i, factor):
        total = m.dp_f[i][d]
        dp_all(i).wait_recv()
        for k in range(1, D):
            total += m.dp_recv[i][k - 1].astype(F32)
        fin = (total * factor).astype(BF)
        m.fin[i][...] = fin
        for j, cc in peers:
            ag_copy(i, j, cc).start()
        put(i, s, fin.astype(F32))

    for i in range(len(pieces)):
        dp_stage(i)
    if Z:
        z_all = whole(m.z_send.at[0:D - 1], m.z_recv, m.z_s, m.z_r)
        z_all.wait_recv()
        total = m.z_f[d]
        for k in range(1, D):
            total += m.z_recv[k - 1].astype(F32)
        m.z_ag[chip] = total.astype(BF)
        for j in range(1, K):
            z_share(j).start()

    small = m.small_dp[...]
    small_dp_all = whole(m.small_dp_recv, m.small_dp_recv, m.smd_s, m.smd_r)
    small_dp_all.wait_recv()
    for k in range(1, D):
        small += m.small_dp_recv[k - 1]
    factor = F32(cfg.tokens) / small[groups:groups + 1, 0:1]
    m.small_fin[...] = small * factor

    def small_ag_copy(j, cc):
        return copy(m.small_fin, m.small_ag.at[2 * j + cc - 1], m.sma_s, m.sma_r,
                    d, 2 * chips[j] + other(cc))

    for j, cc in peers:
        small_ag_copy(j, cc).start()

    for i in range(len(pieces)):
        gather(i, factor)

    def put_gain(q, value):
        for n in range(groups):
            m.gain_out[:, cols(q * F + n * LANES, LANES)] = value[n:n + 1, :]

    def put_z(core, total):
        for q in range(K):
            where = cols((2 * q + core) * F, Z)
            for r in range(R):
                m.up_out[r, :, where] = total[q * R + r:q * R + r + 1]

    if Z:
        z_shared = whole(m.z_ag.at[0:K - 1], m.z_ag.at[0:K - 1], m.zag_s, m.zag_r)
        z_shared.wait_recv()
        total = m.z_ag[0].astype(F32)
        for q in range(1, K):
            total += m.z_ag[q].astype(F32)
        m.zx_send[...] = total
        zx_copy = sib_copy(m.zx_send, m.zx_recv, 8)
        zx_copy.start()
        put_z(c, total * factor)
    put_gain(s, m.small_fin[...])
    small_ag_all = whole(m.small_ag, m.small_ag, m.sma_s, m.sma_r)
    small_ag_all.wait_recv()
    for j, cc in peers:
        put_gain(2 * frm(j) + other(cc), m.small_ag[2 * j + cc - 1])
    if Z:
        zx_copy.wait_recv()
        put_z(1 - c, m.zx_recv[...] * factor)
    for i in range(len(pieces)):
        ag_all(i).wait_recv()
        for j, cc in peers:
            put(i, 2 * frm(j) + other(cc), m.ag[i][2 * j + cc - 1].astype(F32))

    pos_copy(c).wait_send()
    valid_copy(c).wait_send()
    whole(m.cot_src, m.cot_src, m.cot_s, m.cot_r.at[0, 0]).wait_send()
    if Z:
        z_all.wait_send()
        z_shared.wait_send()
        zx_copy.wait_send()
    for group in (sib_proj, sib_act, sq_copy, red_copy, base_copy, back_copy,
                  raise_all, lower_all, small_all, small_dp_all, small_ag_all):
        group.wait_send()
    for i in range(len(pieces)):
        whole(m.rs_send[i], m.rs_recv[i], m.rs_s.at[i], m.rs_r.at[i]).wait_send()
        dp_all(i).wait_send()
        ag_all(i).wait_send()


def write_out(*refs):
    n = len(refs) // 2
    copies = [pltpu.make_async_copy(refs[i], refs[n + i], refs[2 * n].at[i]) for i in range(n)]
    for copy in copies:
        copy.start()
    for copy in copies:
        copy.wait()


def block_width(M, S):
    width = -(-M // (LANES * S)) * LANES
    while M % (2 * width):
        width += LANES
    return width


def shards(projections, rotated_query_gradient, gains, adapter_lowering, adapter_raising,
           activations, positions, valid):
    D, S = lax.axis_size("dp"), lax.axis_size("seq")
    T, QF = projections.shape[2:]
    F = rotated_query_gradient.shape[3]
    R, M = adapter_lowering.shape[1:]
    W = block_width(M, S)
    KD = M // (2 * W)
    RP = -(-R // 16) * 16
    K = S // 2
    T2 = 2 * T
    ranks = D * R
    folded = -(-K * R // 16) * 16
    first = -(-W // (2 * LANES)) * LANES
    Z = F * 3 // (4 * LANES) * LANES if F >= 512 else 0
    pieces = [("d", 0, first)] + ([("d", first, W - first)] if W > first else []) + [("u", Z, F - Z)]
    cfg = SimpleNamespace(S=S, D=D, T=T, F=F, W=W, R=R, RP=RP, M=M, QF=QF, KD=KD, Z=Z,
                          tokens=D * S * T, pieces=pieces)

    hw = 256 if F % 256 == 0 else 128
    small_rows = -(-(F // LANES + 1) // 8) * 8
    vmem = pltpu.VMEM
    dma = pltpu.SemaphoreType.DMA
    scratch = dict(
        p2=vmem((T2, K * F), BF),
        a2=vmem((T2, K * W), BF),
        cot=vmem((K, T2, F), BF),
        cot_src=vmem((K - 1, T2, F), BF),
        low=vmem((R, M), BF),
        rai=vmem((R, QF), BF),
        pos=vmem((2, 3, 1, T), jnp.int32),
        valid=vmem((2, 1, T), jnp.int32),
        freq=vmem((1, LANES), F32),
        gains=vmem((1, QF), F32),
        swap=vmem((hw, hw), BF),
        fold=vmem((folded, W + F), F32),
        packed_r=vmem((D, folded, F), BF),
        packed_l=vmem((D, folded, W), BF),
        adaptf_r=vmem((K, ranks, F), F32),
        adaptf_l=vmem((K, ranks, W), F32),
        adapt_r=vmem((K, ranks, F), BF),
        adapt_l=vmem((K, ranks, W), BF),
        scaled=vmem((K, T2, F), F32),
        cos=vmem((T2, LANES), F32),
        sin=vmem((T2, LANES), F32),
        inv=vmem((T2, LANES), F32),
        coef=vmem((T2, LANES), F32),
        sq_send=vmem((T2, LANES), F32),
        sq_recv=vmem((T2, LANES), F32),
        dot=vmem((T2, LANES), F32),
        inv_row=vmem((1, T2), F32),
        base=vmem((ranks, T2), F32),
        base_send=vmem((ranks, T2), F32),
        base_recv=vmem((ranks, T2), F32),
        red_send=vmem((ranks, T2), F32),
        red_recv=vmem((ranks, T2), F32),
        back_send=vmem((ranks + 8, T2), F32),
        back_recv=vmem((ranks + 8, T2), F32),
        redt=vmem((ranks, T2), BF),
        backt=vmem((ranks, T2), BF),
        small_send=vmem((K, small_rows, LANES), F32),
        small_recv=vmem((K - 1, small_rows, LANES), F32),
        small_dp=vmem((small_rows, LANES), F32),
        small_dp_recv=vmem((D - 1, small_rows, LANES), F32),
        small_fin=vmem((small_rows, LANES), F32),
        small_ag=vmem((S - 1, small_rows, LANES), F32),
    )
    if Z:
        scratch.update(
            z_term=vmem((K, ranks, Z), F32),
            z_f=vmem((D, folded, Z), F32),
            z_send=vmem((D, folded, Z), BF),
            z_recv=vmem((D - 1, folded, Z), BF),
            z_ag=vmem((K, folded, Z), BF),
            zx_send=vmem((folded, Z), F32),
            zx_recv=vmem((folded, Z), F32),
        )
    for kind, off, width in pieces:
        for name, value in dict(
            rs_send=vmem((K - 1, ranks, width), BF),
            rs_recv=vmem((K - 1, ranks, width), BF),
            own=vmem((ranks, width), F32),
            tot=vmem((ranks + RP, width), F32),
            dp_f=vmem((D, RP, width), F32),
            dp_send=vmem((D, RP, width), BF),
            dp_recv=vmem((D - 1, RP, width), BF),
            fin=vmem((RP, width), BF),
            ag=vmem((S - 1, RP, width), BF),
        ).items():
            scratch.setdefault(name, []).append(value)
    n = len(pieces)
    sems = dict(
        local_sem=(10 + K,), cot_s=(), cot_r=(K, 2), ar_s=(), ar_r=(), al_s=(), al_r=(), sib_s=(9,), sib_r=(9,),
        sm_s=(), sm_r=(), smd_s=(), smd_r=(), sma_s=(), sma_r=(),
        z_s=(), z_r=(), zag_s=(), zag_r=(), rs_s=(n,), rs_r=(n,), dp_s=(n,), dp_r=(n,), ag_s=(n,), ag_r=(n,),
    )
    scratch.update({name: dma(shape) if shape else dma for name, shape in sems.items()})
    hbm = pl.BlockSpec(memory_space=pltpu.HBM)
    inputs = dict(
        proj_hbm=projections.reshape(T, QF),
        cot_hbm=rotated_query_gradient.reshape(K, T2, F),
        act_hbm=activations.reshape(T, M),
        low_hbm=adapter_lowering[0],
        rai_hbm=adapter_raising[0],
        gains_hbm=gains,
        freq_hbm=jnp.asarray(lane_frequencies()),
        pos_hbm=positions,
        valid_hbm=valid.reshape(1, T),
    )
    outputs = dict(
        down_out=jax.ShapeDtypeStruct((R, 1, M), F32),
        up_out=jax.ShapeDtypeStruct((R, 1, QF), F32),
        gain_out=jax.ShapeDtypeStruct((1, QF), F32),
    )
    leaves, tree = jax.tree.flatten([inputs, outputs, scratch])
    count = len(inputs) + len(outputs)
    results = pl.pallas_call(
        functools.partial(kernel, cfg, tree),
        out_shape=leaves[len(inputs):count],
        in_specs=[hbm] * len(inputs),
        out_specs=[pl.BlockSpec(memory_space=vmem)] * len(outputs),
        scratch_shapes=leaves[count:],
        compiler_params=pltpu.CompilerParams(
            collective_id=0, has_side_effects=True, vmem_limit_bytes=40 * 1024 * 1024
        ),
    )(*[pltpu.with_memory_space_constraint(x, pltpu.HBM) for x in leaves[:len(inputs)]])
    results = pl.pallas_call(
        write_out,
        out_shape=leaves[len(inputs):count],
        in_specs=[pl.BlockSpec(memory_space=vmem)] * len(outputs),
        out_specs=[hbm] * len(outputs),
        scratch_shapes=[dma((len(outputs),))],
        compiler_params=pltpu.CompilerParams(vmem_limit_bytes=1024 * 1024),
    )(*results)
    down, gain, up = results
    return down.reshape(1, R, M), up.reshape(1, R, QF), gain


def solution(mesh):
    in_specs = (
        P(None, "dp", "seq", None),
        P(None, "dp", None, "seq"),
        P(),
        P(None, "dp", None),
        P(None, "dp", None),
        P("dp", "seq", None),
        P(None, "dp", "seq"),
        P("dp", "seq"),
    )
    out_specs = (P(None, "dp", None), P(None, "dp", None), P())
    return jax.shard_map(shards, mesh=mesh, in_specs=in_specs, out_specs=out_specs, check_vma=False)
```

```python
import functools
from types import SimpleNamespace

import jax
import jax.numpy as jnp
import numpy as np
from jax import lax
from jax.experimental import pallas as pl
from jax.experimental.pallas import tpu as pltpu
from jax.sharding import PartitionSpec as P

HD = 128
EPSILON = 1e-06
LANES = 128
BF = jnp.bfloat16
F32 = jnp.float32
MESH = pl.DeviceIdType.MESH
NT = (((1,), (1,)), ((), ()))


def group_counts():
    one_sixth = HD // 6
    return (HD // 2 - 2 * one_sixth, one_sixth, one_sixth)


def lane_frequencies():
    pieces = []
    for n in group_counts():
        pieces.append(np.float32(10000.0) ** (-np.arange(n, dtype=np.float32) / np.float32(n)))
    return np.repeat(np.concatenate(pieces).astype(np.float32), 2)[None]


def kernel(cfg, tree, *refs):
    inputs, outputs, scratch = jax.tree.unflatten(tree, refs)
    m = SimpleNamespace(**inputs, **outputs, **scratch)
    S, D, T, F, W = cfg.S, cfg.D, cfg.T, cfg.F, cfg.W
    R, M, QF, KD, Z = cfg.R, cfg.M, cfg.QF, cfg.KD, cfg.Z
    pieces = cfg.pieces
    K = S // 2
    T2 = 2 * T
    ranks = D * R
    groups = F // LANES
    hw = 256 if F % 256 == 0 else 128
    pow2 = K & (K - 1) == 0
    d = lax.axis_index("dp")
    s = lax.axis_index("seq")
    c = lax.rem(s, 2)
    chip = s // 2
    sib = s + 1 - 2 * c
    par = 1 - c

    def to(j):
        if j == 0:
            return chip
        if not pow2:
            return lax.rem(chip + j, K)
        k, bit = chip, 1
        while bit < K:
            if j & bit:
                k = k + bit * (1 - 2 * lax.rem(chip // bit, 2))
            bit *= 2
        return k

    def slot(j):
        return j if pow2 else (K - j) % K

    chips = [to(j) for j in range(K)]

    def frm(j):
        return chips[slot(j)]

    def cols(start, width):
        return pl.ds(pl.multiple_of(start, LANES), width)

    def rows(core):
        return pl.ds(pl.multiple_of(core * T, T), T)

    def copy(src, dst, ss, rs, dp, seq):
        return pltpu.make_async_remote_copy(
            src_ref=src, dst_ref=dst, send_sem=ss, recv_sem=rs,
            device_id=(dp, seq), device_id_type=MESH,
        )

    def other(cc):
        return c if cc == 0 else 1 - c

    peers = [(j, cc) for j in reversed(range(K)) for cc in range(2) if (j, cc) != (0, 0)]

    barrier = pltpu.get_barrier_semaphore()
    for j, cc in peers:
        pl.semaphore_signal(barrier, inc=1, device_id=(d, 2 * chips[j] + other(cc)), device_id_type=MESH)
    for k in range(1, D):
        pl.semaphore_signal(barrier, inc=1, device_id=(lax.rem(d + k, D), s), device_id_type=MESH)

    def local(src, dst, i):
        return pltpu.make_async_copy(src, dst, m.local_sem.at[i])

    low_load = local(m.low_hbm, m.maps.at[:, 0:M], 0)
    rai_load = local(m.rai_hbm, m.maps.at[:, M:M + QF], 0)
    pos_load = local(m.pos_hbm, m.marks.at[c, 0:3], 1)
    valid_load = local(m.valid_hbm, m.marks.at[c, 3], 1)
    freq_load = local(m.freq_hbm, m.lines.at[:, 0:LANES], 2)
    gains_load = local(m.gains_hbm, m.lines.at[:, LANES:LANES + QF], 2)
    cot_loads = [local(m.cot_hbm.at[chips[j]], m.cot_src.at[j - 1], 4 + j) for j in range(1, K)]
    proj_loads = [
        local(m.proj_hbm.at[:, cols((2 * k + par) * F, F)], m.p2.at[rows(c), pl.ds(k * F, F)], 3)
        for k in range(K)
    ]
    act_loads = [
        local(m.act_hbm.at[:, cols((2 * k + par) * W, W)], m.a2.at[rows(c), pl.ds(k * W, W)], 4)
        for k in range(KD)
    ]
    for j in range(1, K):
        cot_loads[j - 1].start()
    low_load.start()
    rai_load.start()
    pos_load.start()
    valid_load.start()
    freq_load.start()
    gains_load.start()
    for load in proj_loads + act_loads:
        load.start()

    def cot_copy(j, r):
        part = pl.ds(r * T, T)
        return copy(m.cot_src.at[j - 1, part], m.cot.at[j, part],
                    m.cot_s, m.cot_r.at[j - 1, r], d, 2 * chips[j] + par)

    def raise_copy(k):
        return copy(m.packed_r.at[d], m.packed_r.at[d], m.ar_s, m.ar_r, lax.rem(d + k, D), s)

    def lower_copy(k):
        return copy(m.packed_l.at[d], m.packed_l.at[d], m.al_s, m.al_r, lax.rem(d + k, D), s)

    def sib_copy(src, dst, i):
        return copy(src, dst, m.sib_s.at[i], m.sib_r.at[i], d, sib)

    def own_copy():
        return sib_copy(m.cot_hbm.at[chip], m.cot.at[0], 6)

    def pos_copy(core):
        return sib_copy(m.pos_hbm, m.marks.at[core, 0:3], 0)

    def valid_copy(core):
        return sib_copy(m.valid_hbm, m.marks.at[core, 3], 0)

    def proj_copy(k, core):
        return sib_copy(m.proj_hbm.at[:, cols((2 * k + c) * F, F)],
                        m.p2.at[rows(core), pl.ds(k * F, F)], 6)

    def act_copy(k, core):
        return sib_copy(m.act_hbm.at[:, cols((2 * k + c) * W, W)],
                        m.a2.at[rows(core), pl.ds(k * W, W)], 7)

    def xch_copy(send, recv, i):
        return sib_copy(send, recv, i)

    sq_copy = xch_copy(m.sq_send, m.sq_recv, 2)
    red_copy = xch_copy(m.red_send, m.red_recv, 3)
    base_copy = xch_copy(m.base_send, m.base_recv, 4)
    back_copy = xch_copy(m.back_send, m.back_recv, 5)

    near = [j for j in range(1, K) if pow2 and j & (j - 1) == 0]
    far = [j for j in range(1, K) if j not in near]
    order = [(j, r) for r in range(2) for j in near] + [(j, r) for j in far for r in range(2)]

    pl.semaphore_wait(barrier, S + D - 2)
    pos_copy(c).start()
    valid_copy(c).start()
    for j in near:
        cot_loads[j - 1].wait()
        cot_copy(j, 0).start()
    for j in near:
        cot_copy(j, 1).start()
    for j in far:
        cot_loads[j - 1].wait()

    for j in far:
        for r in range(2):
            cot_copy(j, r).start()
    own_copy().start()
    fold = m.fold
    if fold.shape[0] > K * R or KD < K:
        fold[...] = jnp.zeros_like(fold)
    if KD < K:
        m.a2[:, KD * W:] = jnp.zeros((T2, (K - KD) * W), BF)
    local(m.maps, m.maps, 0).wait()
    for q in range(K):
        if q < KD:
            fold[q * R:(q + 1) * R, 0:W] = m.maps[:, cols((2 * q + par) * W, W)].astype(F32)
        fold[q * R:(q + 1) * R, W:W + F] = m.maps[:, cols(M + (2 * q + par) * F, F)].astype(F32)
    m.packed_r[d] = fold[:, W:].astype(BF)
    m.packed_l[d] = fold[:, :W].astype(BF)

    for k in range(1, D):
        raise_copy(k).start()
    for k in range(1, D):
        lower_copy(k).start()
    for k in range(K):
        proj_copy(k, c).start()
    for k in range(KD):
        act_copy(k, c).start()

    row_i = lax.broadcasted_iota(jnp.int32, (hw, hw), 0)
    col_i = lax.broadcasted_iota(jnp.int32, (hw, hw), 1)
    even = lax.rem(col_i, 2) == 0
    m.swap[...] = jnp.where(
        even & (row_i == col_i + 1), 1.0, jnp.where(jnp.logical_not(even) & (row_i == col_i - 1), -1.0, 0.0)
    ).astype(BF)

    local(m.marks.at[c], m.marks.at[c], 1).wait()
    local(m.lines, m.lines, 2).wait()
    sib_marks = sib_copy(m.marks.at[c], m.marks.at[1 - c], 0)
    sib_marks.wait_recv()
    n0, n1, _ = group_counts()
    lane = lax.broadcasted_iota(jnp.int32, (T, LANES), 1)

    def column(row):
        return jnp.broadcast_to(row.astype(F32), (LANES, T)).T

    count = jnp.zeros((1, 1), F32)
    for h in range(2):
        index = jnp.where(
            lane < 2 * n0, column(m.marks[h, 0]),
            jnp.where(lane < 2 * (n0 + n1), column(m.marks[h, 1]), column(m.marks[h, 2])),
        )
        angle = index * m.lines[:, 0:LANES]
        ok = column(m.marks[h, 3])
        m.cos[h * T:(h + 1) * T, :] = jnp.cos(angle) * ok
        m.sin[h * T:(h + 1) * T, :] = jnp.sin(angle) * ok
        count += jnp.sum(m.marks[h, 3].astype(F32), axis=1, keepdims=True)
    m.small_send[...] = jnp.broadcast_to(count[:, :, None], m.small_send.shape)

    proj_all = m.proj_hbm.at[:, 0:K * F]
    local(proj_all, m.p2.at[rows(c)], 3).wait()
    sib_proj = sib_copy(m.cot.at[0:(K + 2) // 2], m.cot.at[0:(K + 2) // 2], 6)
    sib_proj.wait_recv()
    square = jnp.zeros((T2, LANES), F32)
    for i in range(K * groups):
        v = m.p2[:, i * LANES:(i + 1) * LANES].astype(F32)
        square += v * v
    m.sq_send[...] = square
    sq_copy.start()
    m.dot[...] = jnp.zeros_like(m.dot)
    sq_copy.wait_recv()
    square = m.sq_send[...] + m.sq_recv[...]
    inverse = lax.rsqrt(jnp.sum(square, axis=1, keepdims=True) / QF + EPSILON)
    inverse = jnp.broadcast_to(inverse, (T2, LANES))
    m.inv[...] = inverse
    m.inv_row[...] = inverse.T[0:1, :]

    def wide(x):
        return jnp.concatenate([x] * (hw // LANES), axis=1) if hw > LANES else x

    def chunk(j, r):
        k = frm(j)
        part = slice(r * T, (r + 1) * T)
        inv = wide(m.inv[part])
        cw, sw = wide(m.cos[part]), wide(m.sin[part])
        for i in range(F // hw):
            x = m.cot[j, part, i * hw:(i + 1) * hw]
            xs = jnp.dot(x, m.swap[...], preferred_element_type=F32)
            un = cw * x.astype(F32) + sw * xs
            prod = un * (m.p2[part, cols(k * F + i * hw, hw)].astype(F32) * inv)
            g = jnp.sum(prod, axis=0, keepdims=True)
            for t in range(hw // LANES):
                n = i * (hw // LANES) + t
                piece = g[:, t * LANES:(t + 1) * LANES]
                if r > 0:
                    piece += m.small_send[j, n:n + 1, :]
                m.small_send[j, n:n + 1, :] = piece
            gn = m.lines[:, cols(LANES + (2 * k + par) * F + i * hw, hw)]
            m.scaled[j, part, i * hw:(i + 1) * hw] = un * gn * inv
            pg = prod * gn
            acc = pg[:, :LANES]
            for t in range(1, hw // LANES):
                acc += pg[:, t * LANES:(t + 1) * LANES]
            m.dot[part] += acc

    def whole(src, dst, ss, rs):
        return copy(src, dst, ss, rs, d, sib)

    def unfold(packed, adaptf, adapt):
        for e in range(D):
            fold[:, :packed.shape[2]] = packed[e].astype(F32)
            for q in range(K):
                adaptf[q, e * R:(e + 1) * R, :] = fold[q * R:(q + 1) * R, :packed.shape[2]]
        for q in range(K):
            adapt[q] = adaptf[q].astype(BF)

    def back_part(j, r):
        part = slice(r * T, (r + 1) * T)
        raising = m.adapt_r[frm(j)]
        value = m.scaled[j, part, :]
        high = value.astype(BF)
        low = (value - high.astype(F32)).astype(BF)
        term = lax.dot_general(raising, high, NT, preferred_element_type=F32)
        return term + lax.dot_general(raising, low, NT, preferred_element_type=F32)

    chunk(0, 0)
    chunk(0, 1)
    split = 2 * len(near)
    for j, r in order[:split]:
        cot_copy(j, r).wait_recv()
        chunk(j, r)
    raise_all = whole(m.packed_r.at[0:D - 1], m.packed_r.at[0:D - 1], m.ar_s, m.ar_r)
    raise_all.wait_recv()
    unfold(m.packed_r, m.adaptf_r, m.adapt_r)
    base = jnp.zeros((ranks, T2), F32)
    for k in range(K):
        base += lax.dot_general(m.adapt_r[k], m.p2[:, k * F:(k + 1) * F], NT, preferred_element_type=F32)
    m.base_send[...] = base
    base_copy.start()
    for r in range(2):
        total = jnp.zeros((ranks, T), F32)
        for j in [0] + near:
            total += back_part(j, r)
        m.back_send[0:ranks, r * T:(r + 1) * T] = total

    for j, r in order[split:-1]:
        cot_copy(j, r).wait_recv()
        chunk(j, r)
        m.back_send[0:ranks, r * T:(r + 1) * T] += back_part(j, r)
    lower_all = whole(m.packed_l.at[0:D - 1], m.packed_l.at[0:D - 1], m.al_s, m.al_r)
    lower_all.wait_recv()
    unfold(m.packed_l, m.adaptf_l, m.adapt_l)
    act_all = m.act_hbm.at[:, 0:KD * W]
    local(act_all, m.a2.at[rows(c), 0:KD * W], 4).wait()
    sib_act = sib_copy(act_all, m.a2.at[rows(1 - c), 0:KD * W], 7)
    sib_act.wait_recv()
    red = jnp.zeros((ranks, T2), F32)
    for k in range(KD):
        red += lax.dot_general(m.adapt_l[k], m.a2[:, k * W:(k + 1) * W], NT, preferred_element_type=F32)
    m.red_send[...] = red
    red_copy.start()
    base_copy.wait_recv()
    inv_row = m.inv_row[...]
    m.base[...] = (m.base_send[...] + m.base_recv[...]) * (inv_row * inv_row)

    for j, r in order[-1:]:
        cot_copy(j, r).wait_recv()
        chunk(j, r)
        m.back_send[0:ranks, r * T:(r + 1) * T] += back_part(j, r)
    dot_row = jnp.sum(m.dot[...].T, axis=0, keepdims=True)
    m.back_send[ranks:ranks + 8, :] = jnp.broadcast_to(dot_row, (8, T2))
    back_copy.start()

    def small_copy(j):
        return copy(m.small_send.at[slot(j)], m.small_recv.at[j - 1], m.sm_s, m.sm_r, d, 2 * chips[j] + c)

    for j in range(1, K):
        small_copy(j).start()
    red_copy.wait_recv()
    m.redt[...] = (m.red_send[...] + m.red_recv[...]).astype(BF)
    back_copy.wait_recv()
    back = m.back_send[...] + m.back_recv[...]
    mean_row = back[ranks:ranks + 1, :] / QF
    m.backt[...] = (back[0:ranks, :] - mean_row * m.base[...]).astype(BF)
    mean = jnp.broadcast_to(mean_row, (LANES, T2)).T
    inv = m.inv[...]
    m.coef[...] = inv * inv * mean

    def rs_copy(i, j):
        return copy(m.rs_send[i].at[j - 1], m.rs_recv[i].at[j - 1],
                    m.rs_s.at[i], m.rs_r.at[i], d, 2 * chips[j] + c)

    last = len(pieces) - 1
    def store_term(i, j, lanes, term):
        if j == 0:
            m.own[i][:, lanes] = term
        else:
            m.rs_send[i][j - 1, :, lanes] = term.astype(BF)

    for i, (off, end) in enumerate(pieces):
        width = min(end, W) - off
        if width > 0:
            for j in list(range(1, K)) + [0]:
                values = m.a2[:, cols(chips[j] * W + off, width)]
                store_term(i, j, slice(0, width), jnp.dot(m.backt[...], values, preferred_element_type=F32))
        if i < last:
            for j in far + near:
                rs_copy(i, j).start()

    up_lane = W - pieces[last][0]
    for j in list(range(1, K)) + [0]:
        k = chips[j]
        coef = wide(m.coef[...])
        for i in range(F // hw):
            part = slice(i * hw, (i + 1) * hw)
            p = m.p2[:, cols(k * F + i * hw, hw)].astype(F32)
            delta = (m.scaled[slot(j), :, part] - coef * p).astype(BF)
            term = jnp.dot(m.redt[...], delta, preferred_element_type=F32)
            start = i * hw
            if start < Z:
                m.z_term[k, :, start:min(start + hw, Z)] = term[:, :min(hw, Z - start)]
            if start + hw > Z:
                first = max(start - Z, 0)
                width = start + hw - Z - first
                lanes = slice(up_lane + first, up_lane + first + width)
                store_term(last, j, lanes, term[:, hw - width:])
    for j in far + near:
        rs_copy(last, j).start()

    def z_copy(k):
        return copy(m.z_send.at[lax.rem(d + k, D)], m.z_recv.at[k - 1], m.z_s, m.z_r, lax.rem(d + k, D), sib)

    def z_share(j):
        return copy(m.z_ag.at[chip], m.z_ag.at[chip], m.zag_s, m.zag_r, d, 2 * chips[j] + c)

    if Z:
        for e in range(D):
            for k in range(K):
                m.z_f[e, k * R:(k + 1) * R, :] = m.z_term[k, e * R:(e + 1) * R, :]
            m.z_send[e] = m.z_f[e].astype(BF)
        for k in range(1, D):
            z_copy(k).start()
        z_own = sib_copy(m.z_f.at[d], m.z_own, 1)
        z_own.start()
    small = m.small_send[0]
    small_all = whole(m.small_recv, m.small_recv, m.sm_s, m.sm_r)
    small_all.wait_recv()
    for j in range(1, K):
        small += m.small_recv[j - 1]
    m.small_dp[...] = small

    def small_dp_copy(k):
        return copy(m.small_dp, m.small_dp_recv.at[k - 1], m.smd_s, m.smd_r, lax.rem(d + k, D), s)

    for k in range(1, D):
        small_dp_copy(k).start()

    def dp_copy(i, k):
        return copy(m.dp_send[i].at[lax.rem(d + k, D)], m.dp_recv[i].at[k - 1],
                    m.dp_s.at[i], m.dp_r.at[i], lax.rem(d + k, D), sib)

    def dp_own(i):
        return sib_copy(m.dp_f[i].at[d], m.dp_own[i], 11 + i)

    def dp_stage(i):
        total = m.own[i][...]
        whole(m.rs_send[i], m.rs_recv[i], m.rs_s.at[i], m.rs_r.at[i]).wait_recv()
        for j in range(1, K):
            total += m.rs_recv[i][j - 1].astype(F32)
        tot = m.tot[i]
        tot[...] = total
        for e in range(D):
            for b in range(tot.shape[1] // LANES):
                part = tot[e * R:(e + 1) * R, b * LANES:(b + 1) * LANES]
                m.dp_f[i][e, b * R:(b + 1) * R, :] = part
            m.dp_send[i][e] = m.dp_f[i][e].astype(BF)
        for k in range(1, D):
            dp_copy(i, k).start()
        dp_own(i).start()

    def ag_copy(i, j, cc):
        return copy(m.fin[i], m.ag[i].at[2 * j + cc - 1], m.ag_s.at[i - 1], m.ag_r.at[i - 1],
                    d, 2 * chips[j] + other(cc))

    def put(i, q, value):
        off, end = pieces[i]
        for b in range((end - off) // LANES):
            lane = off + b * LANES
            block = value[b * R:(b + 1) * R]

            def store(out, base, block=block):
                out[:, 0, cols(base, LANES)] = block

            if lane >= W:
                store(m.up_out, q * F + Z + lane - W)
            elif S * W == M:
                store(m.down_out, q * W + lane)
            else:
                base = q * W + lane
                pl.when(base + LANES <= M)(functools.partial(store, m.down_out, base))

    def dp_all(i):
        return whole(m.dp_send[i].at[0:D - 1], m.dp_recv[i], m.dp_s.at[i], m.dp_r.at[i])

    def ag_all(i):
        return whole(m.ag[i], m.ag[i], m.ag_s.at[i - 1], m.ag_r.at[i - 1])

    def ring_copy(j):
        return copy(m.ring.at[chip], m.ring.at[chip], m.ring_s, m.ring_r, d, 2 * chips[j] + c)

    def gather(i, factor):
        dp_own(i).wait_recv()
        total = m.dp_own[i][...]
        dp_all(i).wait_recv()
        for k in range(1, D):
            total += m.dp_recv[i][k - 1].astype(F32)
        fin = (total * factor).astype(BF)
        if i == 0:
            m.ring[chip] = fin
            for j in far + near:
                ring_copy(j).start()
            return
        m.fin[i][...] = fin
        for j, cc in peers:
            ag_copy(i, j, cc).start()
        put(i, s, fin.astype(F32))

    for i in range(len(pieces)):
        dp_stage(i)
    if Z:
        z_all = whole(m.z_send.at[0:D - 1], m.z_recv, m.z_s, m.z_r)
        z_all.wait_recv()
        z_own.wait_recv()
        total = m.z_own[...]
        for k in range(1, D):
            total += m.z_recv[k - 1].astype(F32)
        m.z_ag[chip] = total.astype(BF)
        for j in far + near:
            z_share(j).start()

    small = m.small_dp[...]
    small_dp_all = whole(m.small_dp_recv, m.small_dp_recv, m.smd_s, m.smd_r)
    small_dp_all.wait_recv()
    for k in range(1, D):
        small += m.small_dp_recv[k - 1]
    factor = F32(cfg.tokens) / small[groups:groups + 1, 0:1]
    m.small_ag[chip] = small * factor

    def small_ag_copy(j):
        return copy(m.small_ag.at[chip], m.small_ag.at[chip], m.sma_s, m.sma_r, d, 2 * chips[j] + c)

    for j in far + near:
        small_ag_copy(j).start()

    for i in range(len(pieces)):
        gather(i, factor)

    def put_gain(q, value):
        for n in range(groups):
            m.gain_out[:, cols(q * F + n * LANES, LANES)] = value[n:n + 1, :]

    def put_z(core, total):
        for q in range(K):
            m.up_out[:, 0, cols((2 * q + core) * F, Z)] = total[q * R:(q + 1) * R]

    if Z:
        z_shared = whole(m.z_ag.at[0:K - 1], m.z_ag.at[0:K - 1], m.zag_s, m.zag_r)
        z_shared.wait_recv()
        total = m.z_ag[0].astype(F32)
        for q in range(1, K):
            total += m.z_ag[q].astype(F32)
        m.zx_send[...] = total
        zx_copy = sib_copy(m.zx_send, m.zx_recv, 8)
        zx_copy.start()
        put_z(c, total * factor)
    small_ag_all = whole(m.small_ag.at[0:K - 1], m.small_ag.at[0:K - 1], m.sma_s, m.sma_r)
    small_ag_all.wait_recv()
    small_pass = sib_copy(m.small_ag, m.small_pass, 9)
    small_pass.start()
    for q in range(K):
        put_gain(2 * q + par, m.small_ag[q])
    ring_all = whole(m.ring.at[0:K - 1], m.ring.at[0:K - 1], m.ring_s, m.ring_r)
    ring_all.wait_recv()
    ring_pass = sib_copy(m.ring, m.ring_pass, 10)
    ring_pass.start()
    for q in range(K):
        put(0, 2 * q + c, m.ring[q].astype(F32))
    if Z:
        zx_copy.wait_recv()
        put_z(1 - c, m.zx_recv[...] * factor)
    small_pass.wait_recv()
    for q in range(K):
        put_gain(2 * q + c, m.small_pass[q])
    for i in range(1, len(pieces)):
        ag_all(i).wait_recv()
        for j, cc in peers:
            put(i, 2 * frm(j) + other(cc), m.ag[i][2 * j + cc - 1].astype(F32))
    ring_pass.wait_recv()
    for q in range(K):
        put(0, 2 * q + par, m.ring_pass[q].astype(F32))

    sib_marks.wait_send()
    whole(m.cot_src, m.cot_src, m.cot_s, m.cot_r.at[0, 0]).wait_send()
    if Z:
        z_all.wait_send()
        z_shared.wait_send()
        zx_copy.wait_send()
        z_own.wait_send()
    for group in (sib_proj, sib_act, sq_copy, red_copy, base_copy, back_copy,
                  ring_all, ring_pass, small_pass, raise_all, lower_all, small_all, small_dp_all, small_ag_all):
        group.wait_send()
    for i in range(len(pieces)):
        whole(m.rs_send[i], m.rs_recv[i], m.rs_s.at[i], m.rs_r.at[i]).wait_send()
        dp_all(i).wait_send()
        dp_own(i).wait_send()
        if i > 0:
            ag_all(i).wait_send()


def write_out(*refs):
    n = len(refs) // 2
    copies = [pltpu.make_async_copy(refs[i], refs[n + i], refs[2 * n].at[i]) for i in range(n)]
    for copy in copies:
        copy.start()
    for copy in copies:
        copy.wait()


def block_width(M, S):
    width = -(-M // (LANES * S)) * LANES
    while M % (2 * width):
        width += LANES
    return width


def shards(projections, rotated_query_gradient, gains, adapter_lowering, adapter_raising,
           activations, positions, valid):
    D, S = lax.axis_size("dp"), lax.axis_size("seq")
    T, QF = projections.shape[2:]
    F = rotated_query_gradient.shape[3]
    R, M = adapter_lowering.shape[1:]
    W = block_width(M, S)
    KD = M // (2 * W)
    K = S // 2
    T2 = 2 * T
    ranks = D * R
    folded = -(-K * R // 16) * 16
    Z = F * 3 // (4 * LANES) * LANES if F >= 512 else 0
    starts = list(range(0, W - 2 * LANES + 1, 2 * LANES))
    starts.append(starts[-1] + 2 * LANES if starts else 0)
    pieces = list(zip(starts, starts[1:] + [W + F - Z]))
    cfg = SimpleNamespace(S=S, D=D, T=T, F=F, W=W, R=R, M=M, QF=QF, KD=KD, Z=Z,
                          tokens=D * S * T, pieces=pieces)

    hw = 256 if F % 256 == 0 else 128
    small_rows = -(-(F // LANES + 1) // 8) * 8
    vmem = pltpu.VMEM
    dma = pltpu.SemaphoreType.DMA
    scratch = dict(
        p2=vmem((T2, K * F), BF),
        a2=vmem((T2, K * W), BF),
        cot=vmem((K, T2, F), BF),
        cot_src=vmem((K - 1, T2, F), BF),
        maps=vmem((R, M + QF), BF),
        marks=vmem((2, 4, 1, T), jnp.int32),
        lines=vmem((1, LANES + QF), F32),
        swap=vmem((hw, hw), BF),
        fold=vmem((folded, W + F), F32),
        packed_r=vmem((D, folded, F), BF),
        packed_l=vmem((D, folded, W), BF),
        adaptf_r=vmem((K, ranks, F), F32),
        adaptf_l=vmem((K, ranks, W), F32),
        adapt_r=vmem((K, ranks, F), BF),
        adapt_l=vmem((K, ranks, W), BF),
        scaled=vmem((K, T2, F), F32),
        cos=vmem((T2, LANES), F32),
        sin=vmem((T2, LANES), F32),
        inv=vmem((T2, LANES), F32),
        coef=vmem((T2, LANES), F32),
        sq_send=vmem((T2, LANES), F32),
        sq_recv=vmem((T2, LANES), F32),
        dot=vmem((T2, LANES), F32),
        inv_row=vmem((1, T2), F32),
        base=vmem((ranks, T2), F32),
        base_send=vmem((ranks, T2), F32),
        base_recv=vmem((ranks, T2), F32),
        red_send=vmem((ranks, T2), F32),
        red_recv=vmem((ranks, T2), F32),
        back_send=vmem((ranks + 8, T2), F32),
        back_recv=vmem((ranks + 8, T2), F32),
        redt=vmem((ranks, T2), BF),
        backt=vmem((ranks, T2), BF),
        small_send=vmem((K, small_rows, LANES), F32),
        small_recv=vmem((K - 1, small_rows, LANES), F32),
        small_dp=vmem((small_rows, LANES), F32),
        small_dp_recv=vmem((D - 1, small_rows, LANES), F32),
        small_ag=vmem((K, small_rows, LANES), F32),
        small_pass=vmem((K, small_rows, LANES), F32),
    )
    if Z:
        scratch.update(
            z_term=vmem((K, ranks, Z), F32),
            z_f=vmem((D, folded, Z), F32),
            z_send=vmem((D, folded, Z), BF),
            z_recv=vmem((D - 1, folded, Z), BF),
            z_ag=vmem((K, folded, Z), BF),
            z_own=vmem((folded, Z), F32),
            zx_send=vmem((folded, Z), F32),
            zx_recv=vmem((folded, Z), F32),
        )
    for off, end in pieces:
        width = end - off
        rows = -(-R * (width // LANES) // 8) * 8
        for name, value in dict(
            rs_send=vmem((K - 1, ranks, width), BF),
            rs_recv=vmem((K - 1, ranks, width), BF),
            own=vmem((ranks, width), F32),
            tot=vmem((ranks, width), F32),
            dp_f=vmem((D, rows, LANES), F32),
            dp_send=vmem((D, rows, LANES), BF),
            dp_own=vmem((rows, LANES), F32),
            dp_recv=vmem((D - 1, rows, LANES), BF),
            fin=vmem((rows, LANES), BF),
            ag=vmem((S - 1, rows, LANES), BF),
        ).items():
            scratch.setdefault(name, []).append(value)
    ring = vmem((K, -(-R * (pieces[0][1] // LANES) // 8) * 8, LANES), BF)
    scratch.update(ring=ring, ring_pass=ring)
    n = len(pieces)
    sems = dict(
        local_sem=(4 + K,), cot_s=(), cot_r=(K - 1, 2), ar_s=(), ar_r=(), al_s=(), al_r=(), sib_s=(11 + n,), sib_r=(11 + n,), ring_s=(), ring_r=(),
        sm_s=(), sm_r=(), smd_s=(), smd_r=(), sma_s=(), sma_r=(),
        z_s=(), z_r=(), zag_s=(), zag_r=(), rs_s=(n,), rs_r=(n,), dp_s=(n,), dp_r=(n,), ag_s=(n - 1,), ag_r=(n - 1,),
    )
    scratch.update({name: dma(shape) if shape else dma for name, shape in sems.items()})
    hbm = pl.BlockSpec(memory_space=pltpu.HBM)
    inputs = dict(
        proj_hbm=projections.reshape(T, QF),
        cot_hbm=rotated_query_gradient.reshape(K, T2, F),
        act_hbm=activations.reshape(T, M),
        low_hbm=adapter_lowering[0],
        rai_hbm=adapter_raising[0],
        gains_hbm=gains,
        freq_hbm=jnp.asarray(lane_frequencies()),
        pos_hbm=positions,
        valid_hbm=valid.reshape(1, T),
    )
    outputs = dict(
        down_out=jax.ShapeDtypeStruct((R, 1, M), F32),
        up_out=jax.ShapeDtypeStruct((R, 1, QF), F32),
        gain_out=jax.ShapeDtypeStruct((1, QF), F32),
    )
    leaves, tree = jax.tree.flatten([inputs, outputs, scratch])
    count = len(inputs) + len(outputs)
    results = pl.pallas_call(
        functools.partial(kernel, cfg, tree),
        out_shape=leaves[len(inputs):count],
        in_specs=[hbm] * len(inputs),
        out_specs=[pl.BlockSpec(memory_space=vmem)] * len(outputs),
        scratch_shapes=leaves[count:],
        compiler_params=pltpu.CompilerParams(
            collective_id=0, has_side_effects=True, vmem_limit_bytes=40 * 1024 * 1024
        ),
    )(*[pltpu.with_memory_space_constraint(x, pltpu.HBM) for x in leaves[:len(inputs)]])
    results = pl.pallas_call(
        write_out,
        out_shape=leaves[len(inputs):count],
        in_specs=[pl.BlockSpec(memory_space=vmem)] * len(outputs),
        out_specs=[hbm] * len(outputs),
        scratch_shapes=[dma((len(outputs),))],
        compiler_params=pltpu.CompilerParams(vmem_limit_bytes=1024 * 1024),
    )(*results)
    down, gain, up = results
    return down.reshape(1, R, M), up.reshape(1, R, QF), gain


def solution(mesh):
    in_specs = (
        P(None, "dp", "seq", None),
        P(None, "dp", None, "seq"),
        P(),
        P(None, "dp", None),
        P(None, "dp", None),
        P("dp", "seq", None),
        P(None, "dp", "seq"),
        P("dp", "seq"),
    )
    out_specs = (P(None, "dp", None), P(None, "dp", None), P())
    return jax.shard_map(shards, mesh=mesh, in_specs=in_specs, out_specs=out_specs, check_vma=False)
```

```python
import functools
from types import SimpleNamespace

import jax
import jax.numpy as jnp
import numpy as np
from jax import lax
from jax.experimental import pallas as pl
from jax.experimental.pallas import tpu as pltpu
from jax.sharding import PartitionSpec as P

HD = 128
EPSILON = 1e-06
LANES = 128
BF = jnp.bfloat16
F32 = jnp.float32
MESH = pl.DeviceIdType.MESH
NT = (((1,), (1,)), ((), ()))


def group_counts():
    one_sixth = HD // 6
    return (HD // 2 - 2 * one_sixth, one_sixth, one_sixth)


def lane_frequencies():
    pieces = []
    for n in group_counts():
        pieces.append(np.float32(10000.0) ** (-np.arange(n, dtype=np.float32) / np.float32(n)))
    return np.repeat(np.concatenate(pieces).astype(np.float32), 2)[None]


def kernel(cfg, tree, *refs):
    inputs, outputs, scratch = jax.tree.unflatten(tree, refs)
    m = SimpleNamespace(**inputs, **outputs, **scratch)
    S, D, T, F, W = cfg.S, cfg.D, cfg.T, cfg.F, cfg.W
    R, M, QF, KD, Z = cfg.R, cfg.M, cfg.QF, cfg.KD, cfg.Z
    pieces = cfg.pieces
    K = S // 2
    T2 = 2 * T
    ranks = D * R
    groups = F // LANES
    hw = 256 if F % 256 == 0 else 128
    pow2 = K & (K - 1) == 0
    d = lax.axis_index("dp")
    s = lax.axis_index("seq")
    c = lax.rem(s, 2)
    chip = s // 2
    sib = s + 1 - 2 * c
    par = 1 - c

    def to(j):
        if j == 0:
            return chip
        if not pow2:
            return lax.rem(chip + j, K)
        k, bit = chip, 1
        while bit < K:
            if j & bit:
                k = k + bit * (1 - 2 * lax.rem(chip // bit, 2))
            bit *= 2
        return k

    def slot(j):
        return j if pow2 else (K - j) % K

    chips = [to(j) for j in range(K)]

    def frm(j):
        return chips[slot(j)]

    def cols(start, width):
        return pl.ds(pl.multiple_of(start, LANES), width)

    def rows(core):
        return pl.ds(pl.multiple_of(core * T, T), T)

    def copy(src, dst, ss, rs, dp, seq):
        return pltpu.make_async_remote_copy(
            src_ref=src, dst_ref=dst, send_sem=ss, recv_sem=rs,
            device_id=(dp, seq), device_id_type=MESH,
        )

    def other(cc):
        return c if cc == 0 else 1 - c

    peers = [(j, cc) for j in reversed(range(K)) for cc in range(2) if (j, cc) != (0, 0)]

    barrier = pltpu.get_barrier_semaphore()
    for j, cc in peers:
        pl.semaphore_signal(barrier, inc=1, device_id=(d, 2 * chips[j] + other(cc)), device_id_type=MESH)
    for k in range(1, D):
        pl.semaphore_signal(barrier, inc=1, device_id=(lax.rem(d + k, D), s), device_id_type=MESH)

    def local(src, dst, i):
        return pltpu.make_async_copy(src, dst, m.local_sem.at[i])

    low_load = local(m.low_hbm, m.maps.at[:, 0:M], 0)
    rai_load = local(m.rai_hbm, m.maps.at[:, M:M + QF], 0)
    pos_load = local(m.pos_hbm, m.marks.at[c, 0:3], 1)
    valid_load = local(m.valid_hbm, m.marks.at[c, 3], 1)
    freq_load = local(m.freq_hbm, m.lines.at[:, 0:LANES], 2)
    gains_load = local(m.gains_hbm, m.lines.at[:, LANES:LANES + QF], 2)
    cot_loads = [local(m.cot_hbm.at[chips[j]], m.cot_src.at[j - 1], 4 + j) for j in range(1, K)]
    proj_loads = [
        local(m.proj_hbm.at[:, cols((2 * k + par) * F, F)], m.p2.at[rows(c), pl.ds(k * F, F)], 3)
        for k in range(K)
    ]
    act_loads = [
        local(m.act_hbm.at[:, cols((2 * k + par) * W, W)], m.a2.at[rows(c), pl.ds(k * W, W)], 4)
        for k in range(KD)
    ]
    for j in range(1, K):
        cot_loads[j - 1].start()
    low_load.start()
    rai_load.start()
    pos_load.start()
    valid_load.start()
    freq_load.start()
    gains_load.start()
    for load in proj_loads + act_loads:
        load.start()

    def cot_copy(j, r):
        part = pl.ds(r * T, T)
        return copy(m.cot_src.at[j - 1, part], m.cot.at[j, part],
                    m.cot_s, m.cot_r.at[j - 1, r], d, 2 * chips[j] + par)

    def raise_copy(k):
        return copy(m.packed_r.at[d], m.packed_r.at[d], m.ar_s, m.ar_r, lax.rem(d + k, D), s)

    def lower_copy(k):
        return copy(m.packed_l.at[d], m.packed_l.at[d], m.al_s, m.al_r, lax.rem(d + k, D), s)

    def sib_copy(src, dst, i):
        return copy(src, dst, m.sib_s.at[i], m.sib_r.at[i], d, sib)

    def own_copy():
        return sib_copy(m.cot_hbm.at[chip], m.cot.at[0], 6)

    def pos_copy(core):
        return sib_copy(m.pos_hbm, m.marks.at[core, 0:3], 0)

    def valid_copy(core):
        return sib_copy(m.valid_hbm, m.marks.at[core, 3], 0)

    def proj_copy(k, core):
        return sib_copy(m.proj_hbm.at[:, cols((2 * k + c) * F, F)],
                        m.p2.at[rows(core), pl.ds(k * F, F)], 6)

    def act_copy(k, core):
        return sib_copy(m.act_hbm.at[:, cols((2 * k + c) * W, W)],
                        m.a2.at[rows(core), pl.ds(k * W, W)], 7)

    def xch_copy(send, recv, i):
        return sib_copy(send, recv, i)

    sq_copy = xch_copy(m.sq_send, m.sq_recv, 2)
    red_copy = xch_copy(m.red_send, m.red_recv, 3)
    base_copy = xch_copy(m.base_send, m.base_recv, 4)
    back_copy = xch_copy(m.back_send, m.back_recv, 5)

    near = [j for j in range(1, K) if pow2 and j & (j - 1) == 0]
    far = [j for j in range(1, K) if j not in near]
    order = [(j, r) for r in range(2) for j in near] + [(j, r) for j in far for r in range(2)]

    pl.semaphore_wait(barrier, S + D - 2)
    pos_copy(c).start()
    valid_copy(c).start()
    for j in near:
        cot_loads[j - 1].wait()
        cot_copy(j, 0).start()
    for j in near:
        cot_copy(j, 1).start()
    for j in far:
        cot_loads[j - 1].wait()

    for j in far:
        for r in range(2):
            cot_copy(j, r).start()
    own_copy().start()
    fold = m.fold
    if fold.shape[0] > K * R or KD < K:
        fold[...] = jnp.zeros_like(fold)
    if KD < K:
        m.a2[:, KD * W:] = jnp.zeros((T2, (K - KD) * W), BF)

    local(m.maps, m.maps, 0).wait()
    for q in range(K):
        if q < KD:
            fold[q * R:(q + 1) * R, 0:W] = m.maps[:, cols((2 * q + par) * W, W)].astype(F32)
        fold[q * R:(q + 1) * R, W:W + F] = m.maps[:, cols(M + (2 * q + par) * F, F)].astype(F32)
    m.packed_r[d] = fold[:, W:].astype(BF)
    m.packed_l[d] = fold[:, :W].astype(BF)

    for k in range(1, D):
        raise_copy(k).start()
    for k in range(1, D):
        lower_copy(k).start()
    for k in range(K):
        proj_copy(k, c).start()
    for k in range(KD):
        act_copy(k, c).start()

    row_i = lax.broadcasted_iota(jnp.int32, (hw, hw), 0)
    col_i = lax.broadcasted_iota(jnp.int32, (hw, hw), 1)
    even = lax.rem(col_i, 2) == 0
    m.swap[...] = jnp.where(
        even & (row_i == col_i + 1), 1.0, jnp.where(jnp.logical_not(even) & (row_i == col_i - 1), -1.0, 0.0)
    ).astype(BF)

    local(m.marks.at[c], m.marks.at[c], 1).wait()
    local(m.lines, m.lines, 2).wait()
    sib_marks = sib_copy(m.marks.at[c], m.marks.at[1 - c], 0)
    sib_marks.wait_recv()
    n0, n1, _ = group_counts()
    lane = lax.broadcasted_iota(jnp.int32, (T, LANES), 1)

    def column(row):
        return jnp.broadcast_to(row.astype(F32), (LANES, T)).T

    count = jnp.zeros((1, 1), F32)
    for h in range(2):
        index = jnp.where(
            lane < 2 * n0, column(m.marks[h, 0]),
            jnp.where(lane < 2 * (n0 + n1), column(m.marks[h, 1]), column(m.marks[h, 2])),
        )
        angle = index * m.lines[:, 0:LANES]
        ok = column(m.marks[h, 3])
        m.cos[h * T:(h + 1) * T, :] = jnp.cos(angle) * ok
        m.sin[h * T:(h + 1) * T, :] = jnp.sin(angle) * ok
        count += jnp.sum(m.marks[h, 3].astype(F32), axis=1, keepdims=True)
    m.small_send[...] = jnp.broadcast_to(count[:, :, None], m.small_send.shape)

    proj_all = m.proj_hbm.at[:, 0:K * F]
    local(proj_all, m.p2.at[rows(c)], 3).wait()

    sib_proj = sib_copy(m.cot.at[0:(K + 2) // 2], m.cot.at[0:(K + 2) // 2], 6)
    sib_proj.wait_recv()
    square = jnp.zeros((T2, LANES), F32)
    for i in range(K * groups):
        v = m.p2[:, i * LANES:(i + 1) * LANES].astype(F32)
        square += v * v
    m.sq_send[...] = square
    sq_copy.start()
    m.dot[...] = jnp.zeros_like(m.dot)
    sq_copy.wait_recv()
    square = m.sq_send[...] + m.sq_recv[...]
    inverse = lax.rsqrt(jnp.sum(square, axis=1, keepdims=True) / QF + EPSILON)
    inverse = jnp.broadcast_to(inverse, (T2, LANES))
    m.inv[...] = inverse
    m.inv_row[...] = inverse.T[0:1, :]

    def wide(x):
        return jnp.concatenate([x] * (hw // LANES), axis=1) if hw > LANES else x

    def chunk(j, r):
        k = frm(j)
        part = slice(r * T, (r + 1) * T)
        inv = wide(m.inv[part])
        cw, sw = wide(m.cos[part]), wide(m.sin[part])
        for i in range(F // hw):
            x = m.cot[j, part, i * hw:(i + 1) * hw]
            xs = jnp.dot(x, m.swap[...], preferred_element_type=F32)
            un = cw * x.astype(F32) + sw * xs
            prod = un * (m.p2[part, cols(k * F + i * hw, hw)].astype(F32) * inv)
            g = jnp.sum(prod, axis=0, keepdims=True)
            for t in range(hw // LANES):
                n = i * (hw // LANES) + t
                piece = g[:, t * LANES:(t + 1) * LANES]
                if r > 0:
                    piece += m.small_send[j, n:n + 1, :]
                m.small_send[j, n:n + 1, :] = piece
            gn = m.lines[:, cols(LANES + (2 * k + par) * F + i * hw, hw)]
            m.scaled[j, part, i * hw:(i + 1) * hw] = un * gn * inv
            pg = prod * gn
            acc = pg[:, :LANES]
            for t in range(1, hw // LANES):
                acc += pg[:, t * LANES:(t + 1) * LANES]
            m.dot[part] += acc

    def whole(src, dst, ss, rs):
        return copy(src, dst, ss, rs, d, sib)

    def unfold(packed, adaptf, adapt):
        for e in range(D):
            fold[:, :packed.shape[2]] = packed[e].astype(F32)
            for q in range(K):
                adaptf[q, e * R:(e + 1) * R, :] = fold[q * R:(q + 1) * R, :packed.shape[2]]
        for q in range(K):
            adapt[q] = adaptf[q].astype(BF)

    def back_part(j, r):
        part = slice(r * T, (r + 1) * T)
        raising = m.adapt_r[frm(j)]
        value = m.scaled[j, part, :]
        high = value.astype(BF)
        low = (value - high.astype(F32)).astype(BF)
        term = lax.dot_general(raising, high, NT, preferred_element_type=F32)
        return term + lax.dot_general(raising, low, NT, preferred_element_type=F32)

    chunk(0, 0)
    chunk(0, 1)
    split = 2 * len(near)
    for j, r in order[:split]:
        cot_copy(j, r).wait_recv()
        chunk(j, r)
    raise_all = whole(m.packed_r.at[0:D - 1], m.packed_r.at[0:D - 1], m.ar_s, m.ar_r)
    raise_all.wait_recv()
    unfold(m.packed_r, m.adaptf_r, m.adapt_r)
    base = jnp.zeros((ranks, T2), F32)
    for k in range(K):
        base += lax.dot_general(m.adapt_r[k], m.p2[:, k * F:(k + 1) * F], NT, preferred_element_type=F32)
    m.base_send[...] = base
    base_copy.start()
    for r in range(2):
        total = jnp.zeros((ranks, T), F32)
        for j in [0] + near:
            total += back_part(j, r)
        m.back_send[0:ranks, r * T:(r + 1) * T] = total

    for j, r in order[split:-1]:
        cot_copy(j, r).wait_recv()
        chunk(j, r)
        m.back_send[0:ranks, r * T:(r + 1) * T] += back_part(j, r)
    lower_all = whole(m.packed_l.at[0:D - 1], m.packed_l.at[0:D - 1], m.al_s, m.al_r)
    lower_all.wait_recv()
    unfold(m.packed_l, m.adaptf_l, m.adapt_l)
    act_all = m.act_hbm.at[:, 0:KD * W]
    local(act_all, m.a2.at[rows(c), 0:KD * W], 4).wait()
    sib_act = sib_copy(act_all, m.a2.at[rows(1 - c), 0:KD * W], 7)
    sib_act.wait_recv()
    red = jnp.zeros((ranks, T2), F32)
    for k in range(KD):
        red += lax.dot_general(m.adapt_l[k], m.a2[:, k * W:(k + 1) * W], NT, preferred_element_type=F32)
    m.red_send[...] = red
    red_copy.start()
    base_copy.wait_recv()
    inv_row = m.inv_row[...]
    m.base[...] = (m.base_send[...] + m.base_recv[...]) * (inv_row * inv_row)

    for j, r in order[-1:]:
        cot_copy(j, r).wait_recv()
        chunk(j, r)
        m.back_send[0:ranks, r * T:(r + 1) * T] += back_part(j, r)
    dot_row = jnp.sum(m.dot[...].T, axis=0, keepdims=True)
    m.back_send[ranks:ranks + 8, :] = jnp.broadcast_to(dot_row, (8, T2))
    back_copy.start()

    def small_copy(j):
        return copy(m.small_send.at[slot(j)], m.small_recv.at[j - 1], m.sm_s, m.sm_r, d, 2 * chips[j] + c)

    for j in range(1, K):
        small_copy(j).start()
    red_copy.wait_recv()
    m.redt[...] = (m.red_send[...] + m.red_recv[...]).astype(BF)
    back_copy.wait_recv()
    back = m.back_send[...] + m.back_recv[...]
    mean_row = back[ranks:ranks + 1, :] / QF
    m.backt[...] = (back[0:ranks, :] - mean_row * m.base[...]).astype(BF)
    mean = jnp.broadcast_to(mean_row, (LANES, T2)).T
    inv = m.inv[...]
    m.coef[...] = inv * inv * mean

    def rs_copy(i, j):
        return copy(m.rs_send[i].at[j - 1], m.rs_recv[i].at[j - 1],
                    m.rs_s.at[i], m.rs_r.at[i], d, 2 * chips[j] + c)

    last = len(pieces) - 1
    def store_term(i, j, lanes, term):
        if j == 0:
            m.own[i][:, lanes] = term
        else:
            m.rs_send[i][j - 1, :, lanes] = term.astype(BF)

    for i, (off, end) in enumerate(pieces):
        width = min(end, W) - off
        if width > 0:
            for j in list(range(1, K)) + [0]:
                values = m.a2[:, cols(chips[j] * W + off, width)]
                store_term(i, j, slice(0, width), jnp.dot(m.backt[...], values, preferred_element_type=F32))
        if i < last:
            for j in far + near:
                rs_copy(i, j).start()

    up_lane = W - pieces[last][0]
    for j in list(range(1, K)) + [0]:
        k = chips[j]
        coef = wide(m.coef[...])
        for i in range(F // hw):
            part = slice(i * hw, (i + 1) * hw)
            p = m.p2[:, cols(k * F + i * hw, hw)].astype(F32)
            delta = (m.scaled[slot(j), :, part] - coef * p).astype(BF)
            term = jnp.dot(m.redt[...], delta, preferred_element_type=F32)
            start = i * hw
            if start < Z:
                m.z_term[k, :, start:min(start + hw, Z)] = term[:, :min(hw, Z - start)]
            if start + hw > Z:
                first = max(start - Z, 0)
                width = start + hw - Z - first
                lanes = slice(up_lane + first, up_lane + first + width)
                store_term(last, j, lanes, term[:, hw - width:])
    for j in far + near:
        rs_copy(last, j).start()

    def z_copy(k):
        return copy(m.z_send.at[lax.rem(d + k, D)], m.z_recv.at[k - 1], m.z_s, m.z_r, lax.rem(d + k, D), sib)

    def z_share(j):
        return copy(m.z_ag.at[chip], m.z_ag.at[chip], m.zag_s, m.zag_r, d, 2 * chips[j] + c)

    small = m.small_send[0]
    small_all = whole(m.small_recv, m.small_recv, m.sm_s, m.sm_r)
    small_all.wait_recv()
    for j in range(1, K):
        small += m.small_recv[j - 1]
    m.small_dp[...] = small

    def small_dp_copy(k):
        return copy(m.small_dp, m.small_dp_recv.at[k - 1], m.smd_s, m.smd_r, lax.rem(d + k, D), s)

    for k in range(1, D):
        small_dp_copy(k).start()

    if Z:
        for e in range(D):
            for k in range(K):
                m.z_f[e, k * R:(k + 1) * R, :] = m.z_term[k, e * R:(e + 1) * R, :]
            m.z_send[e] = m.z_f[e].astype(BF)
        for k in range(1, D):
            z_copy(k).start()
        z_own = sib_copy(m.z_f.at[d], m.z_own, 1)
        z_own.start()

    def dp_copy(i, k):
        return copy(m.dp_send[i].at[lax.rem(d + k, D)], m.dp_recv[i].at[k - 1],
                    m.dp_s.at[i], m.dp_r.at[i], lax.rem(d + k, D), sib)

    def dp_own(i):
        return sib_copy(m.dp_f[i].at[d], m.dp_own[i], 11 + i)

    def dp_stage(i):
        total = m.own[i][...]
        whole(m.rs_send[i], m.rs_recv[i], m.rs_s.at[i], m.rs_r.at[i]).wait_recv()
        for j in range(1, K):
            total += m.rs_recv[i][j - 1].astype(F32)
        tot = m.tot[i]
        tot[...] = total
        for e in range(D):
            for b in range(tot.shape[1] // LANES):
                part = tot[e * R:(e + 1) * R, b * LANES:(b + 1) * LANES]
                m.dp_f[i][e, b * R:(b + 1) * R, :] = part
            m.dp_send[i][e] = m.dp_f[i][e].astype(BF)
        for k in range(1, D):
            dp_copy(i, k).start()
        dp_own(i).start()

    def ag_copy(i, j, cc):
        return copy(m.fin[i], m.ag[i].at[2 * j + cc - 1], m.ag_s.at[i - 1], m.ag_r.at[i - 1],
                    d, 2 * chips[j] + other(cc))

    def put(i, q, value):
        off, end = pieces[i]
        for b in range((end - off) // LANES):
            lane = off + b * LANES
            block = value[b * R:(b + 1) * R]

            def store(out, base, block=block):
                out[:, 0, cols(base, LANES)] = block

            if lane >= W:
                store(m.up_out, q * F + Z + lane - W)
            elif S * W == M:
                store(m.down_out, q * W + lane)
            else:
                base = q * W + lane
                pl.when(base + LANES <= M)(functools.partial(store, m.down_out, base))

    def dp_all(i):
        return whole(m.dp_send[i].at[0:D - 1], m.dp_recv[i], m.dp_s.at[i], m.dp_r.at[i])

    def ag_all(i):
        return whole(m.ag[i], m.ag[i], m.ag_s.at[i - 1], m.ag_r.at[i - 1])

    def ring_copy(j):
        return copy(m.ring.at[chip], m.ring.at[chip], m.ring_s, m.ring_r, d, 2 * chips[j] + c)

    def gather(i, factor):
        dp_own(i).wait_recv()
        total = m.dp_own[i][...]
        dp_all(i).wait_recv()
        for k in range(1, D):
            total += m.dp_recv[i][k - 1].astype(F32)
        fin = (total * factor).astype(BF)
        if i == 0:
            m.ring[chip] = fin
            for j in far + near:
                ring_copy(j).start()
            return
        m.fin[i][...] = fin
        for j, cc in peers:
            ag_copy(i, j, cc).start()
        put(i, s, fin.astype(F32))

    for i in range(len(pieces)):
        dp_stage(i)
    if Z:
        z_all = whole(m.z_send.at[0:D - 1], m.z_recv, m.z_s, m.z_r)
        z_all.wait_recv()
        z_own.wait_recv()
        total = m.z_own[...]
        for k in range(1, D):
            total += m.z_recv[k - 1].astype(F32)
        m.z_ag[chip] = total.astype(BF)
        for j in far + near:
            z_share(j).start()

    small = m.small_dp[...]
    small_dp_all = whole(m.small_dp_recv, m.small_dp_recv, m.smd_s, m.smd_r)
    small_dp_all.wait_recv()
    for k in range(1, D):
        small += m.small_dp_recv[k - 1]
    factor = F32(cfg.tokens) / small[groups:groups + 1, 0:1]
    m.small_ag[chip] = small * factor

    def small_ag_copy(j):
        return copy(m.small_ag.at[chip], m.small_ag.at[chip], m.sma_s, m.sma_r, d, 2 * chips[j] + c)

    for j in far + near:
        small_ag_copy(j).start()

    for i in range(len(pieces)):
        gather(i, factor)

    def put_gain(q, value):
        for n in range(groups):
            m.gain_out[:, cols(q * F + n * LANES, LANES)] = value[n:n + 1, :]

    def put_z(core, total):
        for q in range(K):
            m.up_out[:, 0, cols((2 * q + core) * F, Z)] = total[q * R:(q + 1) * R]

    if Z:
        z_shared = whole(m.z_ag.at[0:K - 1], m.z_ag.at[0:K - 1], m.zag_s, m.zag_r)
        z_shared.wait_recv()
        total = m.z_ag[0].astype(F32)
        for q in range(1, K):
            total += m.z_ag[q].astype(F32)
        m.zx_send[...] = total
        zx_copy = sib_copy(m.zx_send, m.zx_recv, 8)
        zx_copy.start()
        put_z(c, total * factor)
    small_ag_all = whole(m.small_ag.at[0:K - 1], m.small_ag.at[0:K - 1], m.sma_s, m.sma_r)
    small_ag_all.wait_recv()
    small_pass = sib_copy(m.small_ag, m.small_pass, 9)
    small_pass.start()
    for q in range(K):
        put_gain(2 * q + par, m.small_ag[q])
    ring_all = whole(m.ring.at[0:K - 1], m.ring.at[0:K - 1], m.ring_s, m.ring_r)
    ring_all.wait_recv()
    ring_pass = sib_copy(m.ring, m.ring_pass, 10)
    ring_pass.start()
    for q in range(K):
        put(0, 2 * q + c, m.ring[q].astype(F32))
    if Z:
        zx_copy.wait_recv()
        put_z(1 - c, m.zx_recv[...] * factor)
    small_pass.wait_recv()
    for q in range(K):
        put_gain(2 * q + c, m.small_pass[q])
    for i in range(1, len(pieces)):
        ag_all(i).wait_recv()
        for j, cc in peers:
            put(i, 2 * frm(j) + other(cc), m.ag[i][2 * j + cc - 1].astype(F32))
    ring_pass.wait_recv()
    for q in range(K):
        put(0, 2 * q + par, m.ring_pass[q].astype(F32))

    sib_marks.wait_send()
    whole(m.cot_src, m.cot_src, m.cot_s, m.cot_r.at[0, 0]).wait_send()
    if Z:
        z_all.wait_send()
        z_shared.wait_send()
        zx_copy.wait_send()
        z_own.wait_send()
    for group in (sib_proj, sib_act, sq_copy, red_copy, base_copy, back_copy,
                  ring_all, ring_pass, small_pass, raise_all, lower_all, small_all, small_dp_all, small_ag_all):
        group.wait_send()
    for i in range(len(pieces)):
        whole(m.rs_send[i], m.rs_recv[i], m.rs_s.at[i], m.rs_r.at[i]).wait_send()
        dp_all(i).wait_send()
        dp_own(i).wait_send()
        if i > 0:
            ag_all(i).wait_send()


def write_out(*refs):
    n = len(refs) // 2
    copies = [pltpu.make_async_copy(refs[i], refs[n + i], refs[2 * n].at[i]) for i in range(n)]
    for copy in copies:
        copy.start()
    for copy in copies:
        copy.wait()


def block_width(M, S):
    width = -(-M // (LANES * S)) * LANES
    while M % (2 * width):
        width += LANES
    return width


def shards(projections, rotated_query_gradient, gains, adapter_lowering, adapter_raising,
           activations, positions, valid):
    D, S = lax.axis_size("dp"), lax.axis_size("seq")
    T, QF = projections.shape[2:]
    F = rotated_query_gradient.shape[3]
    R, M = adapter_lowering.shape[1:]
    W = block_width(M, S)
    KD = M // (2 * W)
    K = S // 2
    T2 = 2 * T
    ranks = D * R
    folded = -(-K * R // 16) * 16
    Z = F * 3 // (4 * LANES) * LANES if F >= 512 else 0
    starts = list(range(0, W - 2 * LANES + 1, 2 * LANES))
    starts.append(starts[-1] + 2 * LANES if starts else 0)
    pieces = list(zip(starts, starts[1:] + [W + F - Z]))
    cfg = SimpleNamespace(S=S, D=D, T=T, F=F, W=W, R=R, M=M, QF=QF, KD=KD, Z=Z,
                          tokens=D * S * T, pieces=pieces)

    hw = 256 if F % 256 == 0 else 128
    small_rows = -(-(F // LANES + 1) // 8) * 8
    vmem = pltpu.VMEM
    dma = pltpu.SemaphoreType.DMA
    scratch = dict(
        p2=vmem((T2, K * F), BF),
        a2=vmem((T2, K * W), BF),
        cot=vmem((K, T2, F), BF),
        cot_src=vmem((K - 1, T2, F), BF),
        maps=vmem((R, M + QF), BF),
        marks=vmem((2, 4, 1, T), jnp.int32),
        lines=vmem((1, LANES + QF), F32),
        swap=vmem((hw, hw), BF),
        fold=vmem((folded, W + F), F32),
        packed_r=vmem((D, folded, F), BF),
        packed_l=vmem((D, folded, W), BF),
        adaptf_r=vmem((K, ranks, F), F32),
        adaptf_l=vmem((K, ranks, W), F32),
        adapt_r=vmem((K, ranks, F), BF),
        adapt_l=vmem((K, ranks, W), BF),
        scaled=vmem((K, T2, F), F32),
        cos=vmem((T2, LANES), F32),
        sin=vmem((T2, LANES), F32),
        inv=vmem((T2, LANES), F32),
        coef=vmem((T2, LANES), F32),
        sq_send=vmem((T2, LANES), F32),
        sq_recv=vmem((T2, LANES), F32),
        dot=vmem((T2, LANES), F32),
        inv_row=vmem((1, T2), F32),
        base=vmem((ranks, T2), F32),
        base_send=vmem((ranks, T2), F32),
        base_recv=vmem((ranks, T2), F32),
        red_send=vmem((ranks, T2), F32),
        red_recv=vmem((ranks, T2), F32),
        back_send=vmem((ranks + 8, T2), F32),
        back_recv=vmem((ranks + 8, T2), F32),
        redt=vmem((ranks, T2), BF),
        backt=vmem((ranks, T2), BF),
        small_send=vmem((K, small_rows, LANES), F32),
        small_recv=vmem((K - 1, small_rows, LANES), F32),
        small_dp=vmem((small_rows, LANES), F32),
        small_dp_recv=vmem((D - 1, small_rows, LANES), F32),
        small_ag=vmem((K, small_rows, LANES), F32),
        small_pass=vmem((K, small_rows, LANES), F32),
    )
    if Z:
        scratch.update(
            z_term=vmem((K, ranks, Z), F32),
            z_f=vmem((D, folded, Z), F32),
            z_send=vmem((D, folded, Z), BF),
            z_recv=vmem((D - 1, folded, Z), BF),
            z_ag=vmem((K, folded, Z), BF),
            z_own=vmem((folded, Z), F32),
            zx_send=vmem((folded, Z), F32),
            zx_recv=vmem((folded, Z), F32),
        )
    for off, end in pieces:
        width = end - off
        rows = -(-R * (width // LANES) // 8) * 8
        for name, value in dict(
            rs_send=vmem((K - 1, ranks, width), BF),
            rs_recv=vmem((K - 1, ranks, width), BF),
            own=vmem((ranks, width), F32),
            tot=vmem((ranks, width), F32),
            dp_f=vmem((D, rows, LANES), F32),
            dp_send=vmem((D, rows, LANES), BF),
            dp_own=vmem((rows, LANES), F32),
            dp_recv=vmem((D - 1, rows, LANES), BF),
            fin=vmem((rows, LANES), BF),
            ag=vmem((S - 1, rows, LANES), BF),
        ).items():
            scratch.setdefault(name, []).append(value)
    ring = vmem((K, -(-R * (pieces[0][1] // LANES) // 8) * 8, LANES), BF)
    scratch.update(ring=ring, ring_pass=ring)
    n = len(pieces)
    sems = dict(
        local_sem=(4 + K,), cot_s=(), cot_r=(K - 1, 2), ar_s=(), ar_r=(), al_s=(), al_r=(), sib_s=(11 + n,), sib_r=(11 + n,), ring_s=(), ring_r=(),
        sm_s=(), sm_r=(), smd_s=(), smd_r=(), sma_s=(), sma_r=(),
        z_s=(), z_r=(), zag_s=(), zag_r=(), rs_s=(n,), rs_r=(n,), dp_s=(n,), dp_r=(n,), ag_s=(n - 1,), ag_r=(n - 1,),
    )
    scratch.update({name: dma(shape) if shape else dma for name, shape in sems.items()})
    hbm = pl.BlockSpec(memory_space=pltpu.HBM)
    inputs = dict(
        proj_hbm=projections.reshape(T, QF),
        cot_hbm=rotated_query_gradient.reshape(K, T2, F),
        act_hbm=activations.reshape(T, M),
        low_hbm=adapter_lowering[0],
        rai_hbm=adapter_raising[0],
        gains_hbm=gains,
        freq_hbm=jnp.asarray(lane_frequencies()),
        pos_hbm=positions,
        valid_hbm=valid.reshape(1, T),
    )
    outputs = dict(
        down_out=jax.ShapeDtypeStruct((R, 1, M), F32),
        up_out=jax.ShapeDtypeStruct((R, 1, QF), F32),
        gain_out=jax.ShapeDtypeStruct((1, QF), F32),
    )
    leaves, tree = jax.tree.flatten([inputs, outputs, scratch])
    count = len(inputs) + len(outputs)
    results = pl.pallas_call(
        functools.partial(kernel, cfg, tree),
        out_shape=leaves[len(inputs):count],
        in_specs=[hbm] * len(inputs),
        out_specs=[pl.BlockSpec(memory_space=vmem)] * len(outputs),
        scratch_shapes=leaves[count:],
        compiler_params=pltpu.CompilerParams(
            collective_id=0, has_side_effects=True, vmem_limit_bytes=40 * 1024 * 1024
        ),
    )(*[pltpu.with_memory_space_constraint(x, pltpu.HBM) for x in leaves[:len(inputs)]])
    results = pl.pallas_call(
        write_out,
        out_shape=leaves[len(inputs):count],
        in_specs=[pl.BlockSpec(memory_space=vmem)] * len(outputs),
        out_specs=[hbm] * len(outputs),
        scratch_shapes=[dma((len(outputs),))],
        compiler_params=pltpu.CompilerParams(vmem_limit_bytes=1024 * 1024),
    )(*results)
    down, gain, up = results
    return down.reshape(1, R, M), up.reshape(1, R, QF), gain


def solution(mesh):
    in_specs = (
        P(None, "dp", "seq", None),
        P(None, "dp", None, "seq"),
        P(),
        P(None, "dp", None),
        P(None, "dp", None),
        P("dp", "seq", None),
        P(None, "dp", "seq"),
        P("dp", "seq"),
    )
    out_specs = (P(None, "dp", None), P(None, "dp", None), P())
    return jax.shard_map(shards, mesh=mesh, in_specs=in_specs, out_specs=out_specs, check_vma=False)
```

```python
import functools
from types import SimpleNamespace

import jax
import jax.numpy as jnp
import numpy as np
from jax import lax
from jax.experimental import pallas as pl
from jax.experimental.pallas import tpu as pltpu
from jax.sharding import PartitionSpec as P

HD = 128
EPSILON = 1e-06
LANES = 128
BF = jnp.bfloat16
F32 = jnp.float32
MESH = pl.DeviceIdType.MESH
NT = (((1,), (1,)), ((), ()))


def group_counts():
    one_sixth = HD // 6
    return (HD // 2 - 2 * one_sixth, one_sixth, one_sixth)


def lane_frequencies():
    pieces = []
    for n in group_counts():
        pieces.append(np.float32(10000.0) ** (-np.arange(n, dtype=np.float32) / np.float32(n)))
    return np.repeat(np.concatenate(pieces).astype(np.float32), 2)[None]


def kernel(cfg, tree, *refs):
    inputs, outputs, scratch = jax.tree.unflatten(tree, refs)
    m = SimpleNamespace(**inputs, **outputs, **scratch)
    S, D, T, F, W = cfg.S, cfg.D, cfg.T, cfg.F, cfg.W
    R, M, QF, KD, Z = cfg.R, cfg.M, cfg.QF, cfg.KD, cfg.Z
    pieces = cfg.pieces
    K = S // 2
    T2 = 2 * T
    ranks = D * R
    groups = F // LANES
    hw = 256 if F % 256 == 0 else 128
    pow2 = K & (K - 1) == 0
    d = lax.axis_index("dp")
    s = lax.axis_index("seq")
    c = lax.rem(s, 2)
    chip = s // 2
    sib = s + 1 - 2 * c
    par = 1 - c

    def to(j):
        if j == 0:
            return chip
        if not pow2:
            return lax.rem(chip + j, K)
        k, bit = chip, 1
        while bit < K:
            if j & bit:
                k = k + bit * (1 - 2 * lax.rem(chip // bit, 2))
            bit *= 2
        return k

    def slot(j):
        return j if pow2 else (K - j) % K

    chips = [to(j) for j in range(K)]

    def frm(j):
        return chips[slot(j)]

    def cols(start, width):
        return pl.ds(pl.multiple_of(start, LANES), width)

    def rows(core):
        return pl.ds(pl.multiple_of(core * T, T), T)

    def copy(src, dst, ss, rs, dp, seq):
        return pltpu.make_async_remote_copy(
            src_ref=src, dst_ref=dst, send_sem=ss, recv_sem=rs,
            device_id=(dp, seq), device_id_type=MESH,
        )

    def other(cc):
        return c if cc == 0 else 1 - c

    peers = [(j, cc) for j in reversed(range(K)) for cc in range(2) if (j, cc) != (0, 0)]

    barrier = pltpu.get_barrier_semaphore()
    for j, cc in peers:
        pl.semaphore_signal(barrier, inc=1, device_id=(d, 2 * chips[j] + other(cc)), device_id_type=MESH)
    for k in range(1, D):
        pl.semaphore_signal(barrier, inc=1, device_id=(lax.rem(d + k, D), s), device_id_type=MESH)

    def local(src, dst, i):
        return pltpu.make_async_copy(src, dst, m.local_sem.at[i])

    low_load = local(m.low_hbm, m.maps.at[:, 0:M], 0)
    rai_load = local(m.rai_hbm, m.maps.at[:, M:M + QF], 0)
    pos_load = local(m.pos_hbm, m.marks.at[c, 0:3], 1)
    valid_load = local(m.valid_hbm, m.marks.at[c, 3], 1)
    freq_load = local(m.freq_hbm, m.lines.at[:, 0:LANES], 2)
    gains_load = local(m.gains_hbm, m.lines.at[:, LANES:LANES + QF], 2)
    cot_loads = [local(m.cot_hbm.at[chips[j]], m.cot_src.at[j - 1], 4 + j) for j in range(1, K)]
    proj_loads = [
        local(m.proj_hbm.at[:, cols((2 * k + par) * F, F)], m.p2.at[rows(c), pl.ds(k * F, F)], 3)
        for k in range(K)
    ]
    act_loads = [
        local(m.act_hbm.at[:, cols((2 * k + par) * W, W)], m.a2.at[rows(c), pl.ds(k * W, W)], 4)
        for k in range(KD)
    ]
    for j in range(1, K):
        cot_loads[j - 1].start()
    low_load.start()
    rai_load.start()
    pos_load.start()
    valid_load.start()
    freq_load.start()
    gains_load.start()
    for load in proj_loads + act_loads:
        load.start()

    def cot_copy(j, r):
        part = pl.ds(r * T, T)
        return copy(m.cot_src.at[j - 1, part], m.cot.at[j, part],
                    m.cot_s, m.cot_r.at[j - 1, r], d, 2 * chips[j] + par)

    def raise_copy(k):
        return copy(m.packed_r.at[d], m.packed_r.at[d], m.ar_s, m.ar_r, lax.rem(d + k, D), s)

    def lower_copy(k):
        return copy(m.packed_l.at[d], m.packed_l.at[d], m.al_s, m.al_r, lax.rem(d + k, D), s)

    def sib_copy(src, dst, i):
        return copy(src, dst, m.sib_s.at[i], m.sib_r.at[i], d, sib)

    def own_copy():
        return sib_copy(m.cot_hbm.at[chip], m.cot.at[0], 6)

    def pos_copy(core):
        return sib_copy(m.pos_hbm, m.marks.at[core, 0:3], 0)

    def valid_copy(core):
        return sib_copy(m.valid_hbm, m.marks.at[core, 3], 0)

    def proj_copy(k, core):
        return sib_copy(m.proj_hbm.at[:, cols((2 * k + c) * F, F)],
                        m.p2.at[rows(core), pl.ds(k * F, F)], 6)

    def act_copy(k, core):
        return sib_copy(m.act_hbm.at[:, cols((2 * k + c) * W, W)],
                        m.a2.at[rows(core), pl.ds(k * W, W)], 7)

    def xch_copy(send, recv, i):
        return sib_copy(send, recv, i)

    sq_copy = xch_copy(m.sq_send, m.sq_recv, 2)
    red_copy = xch_copy(m.red_send, m.red_recv, 3)
    base_copy = xch_copy(m.base_send, m.base_recv, 4)
    back_copy = xch_copy(m.back_send, m.back_recv, 5)

    near = [j for j in range(1, K) if pow2 and j & (j - 1) == 0]
    far = [j for j in range(1, K) if j not in near]
    order = [(j, r) for r in range(2) for j in near] + [(j, r) for j in far for r in range(2)]

    pl.semaphore_wait(barrier, S + D - 2)
    pos_copy(c).start()
    valid_copy(c).start()
    for j in near:
        cot_loads[j - 1].wait()
        cot_copy(j, 0).start()
    for j in near:
        cot_copy(j, 1).start()
    for j in far:
        cot_loads[j - 1].wait()

    for j in far:
        for r in range(2):
            cot_copy(j, r).start()
    own_copy().start()
    fold = m.fold
    if fold.shape[0] > K * R or KD < K:
        fold[...] = jnp.zeros_like(fold)
    if KD < K:
        m.a2[:, KD * W:] = jnp.zeros((T2, (K - KD) * W), BF)

    local(m.maps, m.maps, 0).wait()
    for q in range(K):
        if q < KD:
            fold[q * R:(q + 1) * R, 0:W] = m.maps[:, cols((2 * q + par) * W, W)].astype(F32)
        fold[q * R:(q + 1) * R, W:W + F] = m.maps[:, cols(M + (2 * q + par) * F, F)].astype(F32)
    m.packed_r[d] = fold[:, W:].astype(BF)
    m.packed_l[d] = fold[:, :W].astype(BF)

    for k in range(1, D):
        raise_copy(k).start()
    for k in range(1, D):
        lower_copy(k).start()
    for k in range(K):
        proj_copy(k, c).start()
    for k in range(KD):
        act_copy(k, c).start()

    row_i = lax.broadcasted_iota(jnp.int32, (hw, hw), 0)
    col_i = lax.broadcasted_iota(jnp.int32, (hw, hw), 1)
    even = lax.rem(col_i, 2) == 0
    m.swap[...] = jnp.where(
        even & (row_i == col_i + 1), 1.0, jnp.where(jnp.logical_not(even) & (row_i == col_i - 1), -1.0, 0.0)
    ).astype(BF)

    local(m.marks.at[c], m.marks.at[c], 1).wait()
    local(m.lines, m.lines, 2).wait()
    sib_marks = sib_copy(m.marks.at[c], m.marks.at[1 - c], 0)
    sib_marks.wait_recv()
    n0, n1, _ = group_counts()
    lane = lax.broadcasted_iota(jnp.int32, (T, LANES), 1)

    def column(row):
        return jnp.broadcast_to(row.astype(F32), (LANES, T)).T

    count = jnp.zeros((1, 1), F32)
    for h in range(2):
        index = jnp.where(
            lane < 2 * n0, column(m.marks[h, 0]),
            jnp.where(lane < 2 * (n0 + n1), column(m.marks[h, 1]), column(m.marks[h, 2])),
        )
        angle = index * m.lines[:, 0:LANES]
        ok = column(m.marks[h, 3])
        m.cos[h * T:(h + 1) * T, :] = jnp.cos(angle) * ok
        m.sin[h * T:(h + 1) * T, :] = jnp.sin(angle) * ok
        count += jnp.sum(m.marks[h, 3].astype(F32), axis=1, keepdims=True)
    m.small_send[...] = jnp.broadcast_to(count[:, :, None], m.small_send.shape)

    proj_all = m.proj_hbm.at[:, 0:K * F]
    local(proj_all, m.p2.at[rows(c)], 3).wait()

    sib_proj = sib_copy(m.cot.at[0:(K + 2) // 2], m.cot.at[0:(K + 2) // 2], 6)
    sib_proj.wait_recv()
    square = jnp.zeros((T2, LANES), F32)
    for i in range(K * groups):
        v = m.p2[:, i * LANES:(i + 1) * LANES].astype(F32)
        square += v * v
    m.sq_send[...] = square
    sq_copy.start()
    m.dot[...] = jnp.zeros_like(m.dot)
    sq_copy.wait_recv()
    square = m.sq_send[...] + m.sq_recv[...]
    inverse = lax.rsqrt(jnp.sum(square, axis=1, keepdims=True) / QF + EPSILON)
    inverse = jnp.broadcast_to(inverse, (T2, LANES))
    m.inv[...] = inverse
    m.inv_row[...] = inverse.T[0:1, :]

    def wide(x):
        return jnp.concatenate([x] * (hw // LANES), axis=1) if hw > LANES else x

    def chunk(j, r):
        k = frm(j)
        part = slice(r * T, (r + 1) * T)
        inv = wide(m.inv[part])
        cw, sw = wide(m.cos[part]), wide(m.sin[part])
        for i in range(F // hw):
            x = m.cot[j, part, i * hw:(i + 1) * hw]
            xs = jnp.dot(x, m.swap[...], preferred_element_type=F32)
            un = cw * x.astype(F32) + sw * xs
            prod = un * (m.p2[part, cols(k * F + i * hw, hw)].astype(F32) * inv)
            g = jnp.sum(prod, axis=0, keepdims=True)
            for t in range(hw // LANES):
                n = i * (hw // LANES) + t
                piece = g[:, t * LANES:(t + 1) * LANES]
                if r > 0:
                    piece += m.small_send[j, n:n + 1, :]
                m.small_send[j, n:n + 1, :] = piece
            gn = m.lines[:, cols(LANES + (2 * k + par) * F + i * hw, hw)]
            m.scaled[j, part, i * hw:(i + 1) * hw] = un * gn * inv
            pg = prod * gn
            acc = pg[:, :LANES]
            for t in range(1, hw // LANES):
                acc += pg[:, t * LANES:(t + 1) * LANES]
            m.dot[part] += acc

    def whole(src, dst, ss, rs):
        return copy(src, dst, ss, rs, d, sib)

    def unfold(packed, adaptf, adapt):
        for e in range(D):
            fold[:, :packed.shape[2]] = packed[e].astype(F32)
            for q in range(K):
                adaptf[q, e * R:(e + 1) * R, :] = fold[q * R:(q + 1) * R, :packed.shape[2]]
        for q in range(K):
            adapt[q] = adaptf[q].astype(BF)

    def back_part(j, r):
        part = slice(r * T, (r + 1) * T)
        raising = m.adapt_r[frm(j)]
        value = m.scaled[j, part, :]
        high = value.astype(BF)
        low = (value - high.astype(F32)).astype(BF)
        term = lax.dot_general(raising, high, NT, preferred_element_type=F32)
        return term + lax.dot_general(raising, low, NT, preferred_element_type=F32)

    chunk(0, 0)
    chunk(0, 1)
    split = 2 * len(near)
    for j, r in order[:split]:
        cot_copy(j, r).wait_recv()
        chunk(j, r)
    raise_all = whole(m.packed_r.at[0:D - 1], m.packed_r.at[0:D - 1], m.ar_s, m.ar_r)
    raise_all.wait_recv()
    unfold(m.packed_r, m.adaptf_r, m.adapt_r)
    base = jnp.zeros((ranks, T2), F32)
    for k in range(K):
        base += lax.dot_general(m.adapt_r[k], m.p2[:, k * F:(k + 1) * F], NT, preferred_element_type=F32)
    m.base_send[...] = base
    base_copy.start()
    for r in range(2):
        total = jnp.zeros((ranks, T), F32)
        for j in [0] + near:
            total += back_part(j, r)
        m.back_send[0:ranks, r * T:(r + 1) * T] = total

    for j, r in order[split:-1]:
        cot_copy(j, r).wait_recv()
        chunk(j, r)
        m.back_send[0:ranks, r * T:(r + 1) * T] += back_part(j, r)
    lower_all = whole(m.packed_l.at[0:D - 1], m.packed_l.at[0:D - 1], m.al_s, m.al_r)
    lower_all.wait_recv()
    unfold(m.packed_l, m.adaptf_l, m.adapt_l)
    act_all = m.act_hbm.at[:, 0:KD * W]
    local(act_all, m.a2.at[rows(c), 0:KD * W], 4).wait()
    sib_act = sib_copy(act_all, m.a2.at[rows(1 - c), 0:KD * W], 7)
    sib_act.wait_recv()
    red = jnp.zeros((ranks, T2), F32)
    for k in range(KD):
        red += lax.dot_general(m.adapt_l[k], m.a2[:, k * W:(k + 1) * W], NT, preferred_element_type=F32)
    m.red_send[...] = red
    red_copy.start()
    base_copy.wait_recv()
    inv_row = m.inv_row[...]
    m.base[...] = (m.base_send[...] + m.base_recv[...]) * (inv_row * inv_row)

    for j, r in order[-1:]:
        cot_copy(j, r).wait_recv()
        chunk(j, r)
        m.back_send[0:ranks, r * T:(r + 1) * T] += back_part(j, r)
    dot_row = jnp.sum(m.dot[...].T, axis=0, keepdims=True)
    m.back_send[ranks:ranks + 8, :] = jnp.broadcast_to(dot_row, (8, T2))
    back_copy.start()

    def small_copy(j):
        return copy(m.small_send.at[slot(j)], m.small_recv.at[j - 1], m.sm_s, m.sm_r, d, 2 * chips[j] + c)

    for j in range(1, K):
        small_copy(j).start()
    red_copy.wait_recv()
    m.redt[...] = (m.red_send[...] + m.red_recv[...]).astype(BF)
    back_copy.wait_recv()
    back = m.back_send[...] + m.back_recv[...]
    mean_row = back[ranks:ranks + 1, :] / QF
    m.backt[...] = (back[0:ranks, :] - mean_row * m.base[...]).astype(BF)
    mean = jnp.broadcast_to(mean_row, (LANES, T2)).T
    inv = m.inv[...]
    m.coef[...] = inv * inv * mean

    def rs_copy(i, j):
        return copy(m.rs_send[i].at[j - 1], m.rs_recv[i].at[j - 1],
                    m.rs_s.at[i], m.rs_r.at[i], d, 2 * chips[j] + c)

    last = len(pieces) - 1
    def store_term(i, j, lanes, term):
        if j == 0:
            m.own[i][:, lanes] = term
        else:
            m.rs_send[i][j - 1, :, lanes] = term.astype(BF)

    def down_term(i, j, off, width):
        values = m.a2[:, cols(chips[j] * W + off, width)]
        store_term(i, j, slice(0, width), jnp.dot(m.backt[...], values, preferred_element_type=F32))

    for i, (off, end) in enumerate(pieces):
        width = min(end, W) - off
        if width > 0:
            for j in far + near:
                down_term(i, j, off, width)
        if i < last:
            for j in far + near:
                rs_copy(i, j).start()

    up_lane = W - pieces[last][0]
    for j in list(range(1, K)) + [0]:
        k = chips[j]
        coef = wide(m.coef[...])
        for i in range(F // hw):
            part = slice(i * hw, (i + 1) * hw)
            p = m.p2[:, cols(k * F + i * hw, hw)].astype(F32)
            delta = (m.scaled[slot(j), :, part] - coef * p).astype(BF)
            term = jnp.dot(m.redt[...], delta, preferred_element_type=F32)
            start = i * hw
            if start < Z:
                m.z_term[k, :, start:min(start + hw, Z)] = term[:, :min(hw, Z - start)]
            if start + hw > Z:
                first = max(start - Z, 0)
                width = start + hw - Z - first
                lanes = slice(up_lane + first, up_lane + first + width)
                store_term(last, j, lanes, term[:, hw - width:])
    for j in far + near:
        rs_copy(last, j).start()
    for i, (off, end) in enumerate(pieces):
        if off < W:
            down_term(i, 0, off, min(end, W) - off)

    def z_copy(k):
        return copy(m.z_send.at[lax.rem(d + k, D)], m.z_recv.at[k - 1], m.z_s, m.z_r, lax.rem(d + k, D), sib)

    def z_share(j):
        return copy(m.z_ag.at[chip], m.z_ag.at[chip], m.zag_s, m.zag_r, d, 2 * chips[j] + c)

    small = m.small_send[0]
    small_all = whole(m.small_recv, m.small_recv, m.sm_s, m.sm_r)
    small_all.wait_recv()
    for j in range(1, K):
        small += m.small_recv[j - 1]
    m.small_dp[...] = small

    def small_dp_copy(k):
        return copy(m.small_dp, m.small_dp_recv.at[k - 1], m.smd_s, m.smd_r, lax.rem(d + k, D), s)

    for k in range(1, D):
        small_dp_copy(k).start()

    if Z:
        for e in range(D):
            for k in range(K):
                m.z_f[e, k * R:(k + 1) * R, :] = m.z_term[k, e * R:(e + 1) * R, :]
            m.z_send[e] = m.z_f[e].astype(BF)
        for k in range(1, D):
            z_copy(k).start()
        z_own = sib_copy(m.z_f.at[d], m.z_own, 1)
        z_own.start()

    def dp_copy(i, k):
        return copy(m.dp_send[i].at[lax.rem(d + k, D)], m.dp_recv[i].at[k - 1],
                    m.dp_s.at[i], m.dp_r.at[i], lax.rem(d + k, D), sib)

    def dp_own(i):
        return sib_copy(m.dp_f[i].at[d], m.dp_own[i], 11 + i)

    def dp_stage(i):
        total = m.own[i][...]
        whole(m.rs_send[i], m.rs_recv[i], m.rs_s.at[i], m.rs_r.at[i]).wait_recv()
        for j in range(1, K):
            total += m.rs_recv[i][j - 1].astype(F32)
        tot = m.tot[i]
        tot[...] = total
        for e in range(D):
            for b in range(tot.shape[1] // LANES):
                part = tot[e * R:(e + 1) * R, b * LANES:(b + 1) * LANES]
                m.dp_f[i][e, b * R:(b + 1) * R, :] = part
            m.dp_send[i][e] = m.dp_f[i][e].astype(BF)
        for k in range(1, D):
            dp_copy(i, k).start()
        dp_own(i).start()

    def ag_copy(i, j, cc):
        return copy(m.fin[i], m.ag[i].at[2 * j + cc - 1], m.ag_s.at[i - 1], m.ag_r.at[i - 1],
                    d, 2 * chips[j] + other(cc))

    def put(i, q, value):
        off, end = pieces[i]
        for b in range((end - off) // LANES):
            lane = off + b * LANES
            block = value[b * R:(b + 1) * R]

            def store(out, base, block=block):
                out[:, 0, cols(base, LANES)] = block

            if lane >= W:
                store(m.up_out, q * F + Z + lane - W)
            elif S * W == M:
                store(m.down_out, q * W + lane)
            else:
                base = q * W + lane
                pl.when(base + LANES <= M)(functools.partial(store, m.down_out, base))

    def dp_all(i):
        return whole(m.dp_send[i].at[0:D - 1], m.dp_recv[i], m.dp_s.at[i], m.dp_r.at[i])

    def ag_all(i):
        return whole(m.ag[i], m.ag[i], m.ag_s.at[i - 1], m.ag_r.at[i - 1])

    def ring_copy(j):
        return copy(m.ring.at[chip], m.ring.at[chip], m.ring_s, m.ring_r, d, 2 * chips[j] + c)

    def gather(i, factor):
        dp_own(i).wait_recv()
        total = m.dp_own[i][...]
        dp_all(i).wait_recv()
        for k in range(1, D):
            total += m.dp_recv[i][k - 1].astype(F32)
        fin = (total * factor).astype(BF)
        if i == 0:
            m.ring[chip] = fin
            for j in far + near:
                ring_copy(j).start()
            return
        m.fin[i][...] = fin
        for j, cc in peers:
            ag_copy(i, j, cc).start()
        put(i, s, fin.astype(F32))

    for i in range(len(pieces)):
        dp_stage(i)
    if Z:
        z_all = whole(m.z_send.at[0:D - 1], m.z_recv, m.z_s, m.z_r)
        z_all.wait_recv()
        z_own.wait_recv()
        total = m.z_own[...]
        for k in range(1, D):
            total += m.z_recv[k - 1].astype(F32)
        m.z_ag[chip] = total.astype(BF)
        for j in far + near:
            z_share(j).start()

    small = m.small_dp[...]
    small_dp_all = whole(m.small_dp_recv, m.small_dp_recv, m.smd_s, m.smd_r)
    small_dp_all.wait_recv()
    for k in range(1, D):
        small += m.small_dp_recv[k - 1]
    factor = F32(cfg.tokens) / small[groups:groups + 1, 0:1]
    m.small_ag[chip] = small * factor

    def small_ag_copy(j):
        return copy(m.small_ag.at[chip], m.small_ag.at[chip], m.sma_s, m.sma_r, d, 2 * chips[j] + c)

    for j in far + near:
        small_ag_copy(j).start()

    for i in range(len(pieces)):
        gather(i, factor)

    def put_gain(q, value):
        for n in range(groups):
            m.gain_out[:, cols(q * F + n * LANES, LANES)] = value[n:n + 1, :]

    def put_z(core, total):
        for q in range(K):
            m.up_out[:, 0, cols((2 * q + core) * F, Z)] = total[q * R:(q + 1) * R]

    if Z:
        z_shared = whole(m.z_ag.at[0:K - 1], m.z_ag.at[0:K - 1], m.zag_s, m.zag_r)
        z_shared.wait_recv()
        total = m.z_ag[0].astype(F32)
        for q in range(1, K):
            total += m.z_ag[q].astype(F32)
        m.zx_send[...] = total
        zx_copy = sib_copy(m.zx_send, m.zx_recv, 8)
        zx_copy.start()
        put_z(c, total * factor)
    small_ag_all = whole(m.small_ag.at[0:K - 1], m.small_ag.at[0:K - 1], m.sma_s, m.sma_r)
    small_ag_all.wait_recv()
    small_pass = sib_copy(m.small_ag, m.small_pass, 9)
    small_pass.start()
    for q in range(K):
        put_gain(2 * q + par, m.small_ag[q])
    ring_all = whole(m.ring.at[0:K - 1], m.ring.at[0:K - 1], m.ring_s, m.ring_r)
    ring_all.wait_recv()
    ring_pass = sib_copy(m.ring, m.ring_pass, 10)
    ring_pass.start()
    for q in range(K):
        put(0, 2 * q + c, m.ring[q].astype(F32))
    if Z:
        zx_copy.wait_recv()
        put_z(1 - c, m.zx_recv[...] * factor)
    small_pass.wait_recv()
    for q in range(K):
        put_gain(2 * q + c, m.small_pass[q])
    for i in range(1, len(pieces)):
        ag_all(i).wait_recv()
        for j, cc in peers:
            put(i, 2 * frm(j) + other(cc), m.ag[i][2 * j + cc - 1].astype(F32))
    ring_pass.wait_recv()
    for q in range(K):
        put(0, 2 * q + par, m.ring_pass[q].astype(F32))

    sib_marks.wait_send()
    whole(m.cot_src, m.cot_src, m.cot_s, m.cot_r.at[0, 0]).wait_send()
    if Z:
        z_all.wait_send()
        z_shared.wait_send()
        zx_copy.wait_send()
        z_own.wait_send()
    for group in (sib_proj, sib_act, sq_copy, red_copy, base_copy, back_copy,
                  ring_all, ring_pass, small_pass, raise_all, lower_all, small_all, small_dp_all, small_ag_all):
        group.wait_send()
    for i in range(len(pieces)):
        whole(m.rs_send[i], m.rs_recv[i], m.rs_s.at[i], m.rs_r.at[i]).wait_send()
        dp_all(i).wait_send()
        dp_own(i).wait_send()
        if i > 0:
            ag_all(i).wait_send()


def write_out(*refs):
    n = len(refs) // 2
    copies = [pltpu.make_async_copy(refs[i], refs[n + i], refs[2 * n].at[i]) for i in range(n)]
    for copy in copies:
        copy.start()
    for copy in copies:
        copy.wait()


def block_width(M, S):
    width = -(-M // (LANES * S)) * LANES
    while M % (2 * width):
        width += LANES
    return width


def shards(projections, rotated_query_gradient, gains, adapter_lowering, adapter_raising,
           activations, positions, valid):
    D, S = lax.axis_size("dp"), lax.axis_size("seq")
    T, QF = projections.shape[2:]
    F = rotated_query_gradient.shape[3]
    R, M = adapter_lowering.shape[1:]
    W = block_width(M, S)
    KD = M // (2 * W)
    K = S // 2
    T2 = 2 * T
    ranks = D * R
    folded = -(-K * R // 16) * 16
    Z = F * 3 // (4 * LANES) * LANES if F >= 512 else 0
    starts = list(range(0, W - 2 * LANES + 1, 2 * LANES))
    starts.append(starts[-1] + 2 * LANES if starts else 0)
    pieces = list(zip(starts, starts[1:] + [W + F - Z]))
    cfg = SimpleNamespace(S=S, D=D, T=T, F=F, W=W, R=R, M=M, QF=QF, KD=KD, Z=Z,
                          tokens=D * S * T, pieces=pieces)

    hw = 256 if F % 256 == 0 else 128
    small_rows = -(-(F // LANES + 1) // 8) * 8
    vmem = pltpu.VMEM
    dma = pltpu.SemaphoreType.DMA
    scratch = dict(
        p2=vmem((T2, K * F), BF),
        a2=vmem((T2, K * W), BF),
        cot=vmem((K, T2, F), BF),
        cot_src=vmem((K - 1, T2, F), BF),
        maps=vmem((R, M + QF), BF),
        marks=vmem((2, 4, 1, T), jnp.int32),
        lines=vmem((1, LANES + QF), F32),
        swap=vmem((hw, hw), BF),
        fold=vmem((folded, W + F), F32),
        packed_r=vmem((D, folded, F), BF),
        packed_l=vmem((D, folded, W), BF),
        adaptf_r=vmem((K, ranks, F), F32),
        adaptf_l=vmem((K, ranks, W), F32),
        adapt_r=vmem((K, ranks, F), BF),
        adapt_l=vmem((K, ranks, W), BF),
        scaled=vmem((K, T2, F), F32),
        cos=vmem((T2, LANES), F32),
        sin=vmem((T2, LANES), F32),
        inv=vmem((T2, LANES), F32),
        coef=vmem((T2, LANES), F32),
        sq_send=vmem((T2, LANES), F32),
        sq_recv=vmem((T2, LANES), F32),
        dot=vmem((T2, LANES), F32),
        inv_row=vmem((1, T2), F32),
        base=vmem((ranks, T2), F32),
        base_send=vmem((ranks, T2), F32),
        base_recv=vmem((ranks, T2), F32),
        red_send=vmem((ranks, T2), F32),
        red_recv=vmem((ranks, T2), F32),
        back_send=vmem((ranks + 8, T2), F32),
        back_recv=vmem((ranks + 8, T2), F32),
        redt=vmem((ranks, T2), BF),
        backt=vmem((ranks, T2), BF),
        small_send=vmem((K, small_rows, LANES), F32),
        small_recv=vmem((K - 1, small_rows, LANES), F32),
        small_dp=vmem((small_rows, LANES), F32),
        small_dp_recv=vmem((D - 1, small_rows, LANES), F32),
        small_ag=vmem((K, small_rows, LANES), F32),
        small_pass=vmem((K, small_rows, LANES), F32),
    )
    if Z:
        scratch.update(
            z_term=vmem((K, ranks, Z), F32),
            z_f=vmem((D, folded, Z), F32),
            z_send=vmem((D, folded, Z), BF),
            z_recv=vmem((D - 1, folded, Z), BF),
            z_ag=vmem((K, folded, Z), BF),
            z_own=vmem((folded, Z), F32),
            zx_send=vmem((folded, Z), F32),
            zx_recv=vmem((folded, Z), F32),
        )
    for off, end in pieces:
        width = end - off
        rows = -(-R * (width // LANES) // 8) * 8
        for name, value in dict(
            rs_send=vmem((K - 1, ranks, width), BF),
            rs_recv=vmem((K - 1, ranks, width), BF),
            own=vmem((ranks, width), F32),
            tot=vmem((ranks, width), F32),
            dp_f=vmem((D, rows, LANES), F32),
            dp_send=vmem((D, rows, LANES), BF),
            dp_own=vmem((rows, LANES), F32),
            dp_recv=vmem((D - 1, rows, LANES), BF),
            fin=vmem((rows, LANES), BF),
            ag=vmem((S - 1, rows, LANES), BF),
        ).items():
            scratch.setdefault(name, []).append(value)
    ring = vmem((K, -(-R * (pieces[0][1] // LANES) // 8) * 8, LANES), BF)
    scratch.update(ring=ring, ring_pass=ring)
    n = len(pieces)
    sems = dict(
        local_sem=(4 + K,), cot_s=(), cot_r=(K - 1, 2), ar_s=(), ar_r=(), al_s=(), al_r=(), sib_s=(11 + n,), sib_r=(11 + n,), ring_s=(), ring_r=(),
        sm_s=(), sm_r=(), smd_s=(), smd_r=(), sma_s=(), sma_r=(),
        z_s=(), z_r=(), zag_s=(), zag_r=(), rs_s=(n,), rs_r=(n,), dp_s=(n,), dp_r=(n,), ag_s=(n - 1,), ag_r=(n - 1,),
    )
    scratch.update({name: dma(shape) if shape else dma for name, shape in sems.items()})
    hbm = pl.BlockSpec(memory_space=pltpu.HBM)
    inputs = dict(
        proj_hbm=projections.reshape(T, QF),
        cot_hbm=rotated_query_gradient.reshape(K, T2, F),
        act_hbm=activations.reshape(T, M),
        low_hbm=adapter_lowering[0],
        rai_hbm=adapter_raising[0],
        gains_hbm=gains,
        freq_hbm=jnp.asarray(lane_frequencies()),
        pos_hbm=positions,
        valid_hbm=valid.reshape(1, T),
    )
    outputs = dict(
        down_out=jax.ShapeDtypeStruct((R, 1, M), F32),
        up_out=jax.ShapeDtypeStruct((R, 1, QF), F32),
        gain_out=jax.ShapeDtypeStruct((1, QF), F32),
    )
    leaves, tree = jax.tree.flatten([inputs, outputs, scratch])
    count = len(inputs) + len(outputs)
    results = pl.pallas_call(
        functools.partial(kernel, cfg, tree),
        out_shape=leaves[len(inputs):count],
        in_specs=[hbm] * len(inputs),
        out_specs=[pl.BlockSpec(memory_space=vmem)] * len(outputs),
        scratch_shapes=leaves[count:],
        compiler_params=pltpu.CompilerParams(
            collective_id=0, has_side_effects=True, vmem_limit_bytes=40 * 1024 * 1024
        ),
    )(*[pltpu.with_memory_space_constraint(x, pltpu.HBM) for x in leaves[:len(inputs)]])
    results = pl.pallas_call(
        write_out,
        out_shape=leaves[len(inputs):count],
        in_specs=[pl.BlockSpec(memory_space=vmem)] * len(outputs),
        out_specs=[hbm] * len(outputs),
        scratch_shapes=[dma((len(outputs),))],
        compiler_params=pltpu.CompilerParams(vmem_limit_bytes=1024 * 1024),
    )(*results)
    down, gain, up = results
    return down.reshape(1, R, M), up.reshape(1, R, QF), gain


def solution(mesh):
    in_specs = (
        P(None, "dp", "seq", None),
        P(None, "dp", None, "seq"),
        P(),
        P(None, "dp", None),
        P(None, "dp", None),
        P("dp", "seq", None),
        P(None, "dp", "seq"),
        P("dp", "seq"),
    )
    out_specs = (P(None, "dp", None), P(None, "dp", None), P())
    return jax.shard_map(shards, mesh=mesh, in_specs=in_specs, out_specs=out_specs, check_vma=False)
```
